32 devices in a mesh: wide: 16 (over z, y, core), narrow: 2 (over x).
Axes of the slice: x: 2, y: 2, z: 4, core: 2. Of those that a mesh axis runs over, the one named last changes fastest.
Arguments:
- hidden_in: bfloat16 [16384, 1024], P(('wide', 'narrow')), may hold values from -6 to 6
- segment_ids: int32 [32, 512], P(('wide', 'narrow')), may hold values from 0 to 7, never falling along the last dimension, each value on 1 to 256 neighbouring positions
- expert_ids: int32 [16384, 8], P(('wide', 'narrow')), may hold values from 0 to 15, all different within a row; in each aligned block of 512 rows (0 to 511, 512 to 1023, ...) at most 512 rows name the same one
- attn_gain: float32 [1024], replicated, may hold values from 0.5 to 1.5
- w_query: bfloat16 [1024, 1024], replicated, may hold values from -0.1875 to 0.1875
- w_key: bfloat16 [1024, 512], replicated, may hold values from -0.1875 to 0.1875
- w_value: bfloat16 [1024, 512], replicated, may hold values from -0.1875 to 0.1875
- w_out: bfloat16 [1024, 1024], replicated, may hold values from -0.75 to 0.75
- ffn_gain: float32 [1024], replicated, may hold values from 0.5 to 1.5
- router: bfloat16 [1024, 16], replicated, may hold values from -0.1875 to 0.1875
- w_gate: bfloat16 [16, 1024, 512], P('wide', None, 'narrow'), may hold values from -0.1875 to 0.1875
- w_up: bfloat16 [16, 1024, 512], P('wide', None, 'narrow'), may hold values from -0.1875 to 0.1875
- w_down: bfloat16 [16, 512, 1024], P('wide', 'narrow'), may hold values from -0.75 to 0.75
- grad_out: bfloat16 [16384, 1024], P(('wide', 'narrow')), may hold values from -6 to 6
Outputs:
- hidden_out: bfloat16 [16384, 1024], P(('wide', 'narrow'))
- grad_in: bfloat16 [16384, 1024], P(('wide', 'narrow'))
- grad_attn_gain: float32 [1024], replicated
- grad_query: float32 [1024, 1024], replicated
- grad_key: float32 [1024, 512], replicated
- grad_value: float32 [1024, 512], replicated
- grad_out_proj: float32 [1024, 1024], replicated
- grad_ffn_gain: float32 [1024], replicated
- grad_router: float32 [1024, 16], replicated
- grad_gate: float32 [16, 1024, 512], P('wide', None, 'narrow')
- grad_up: float32 [16, 1024, 512], P('wide', None, 'narrow')
- grad_down: float32 [16, 512, 1024], P('wide', 'narrow')
The draws below stay inside these ranges and needn't reach their ends.
Inputs may be any that keep to these rules, and one draw needn't show every extreme that they name: `segment_ids`: each packed row has 8 documents numbered in order from 0, each of 1 to half of 512 tokens, one of exactly half of 512. `expert_ids`: each token names 8 different experts. Among the 512 tokens of one packed row no expert is named more than 512 times, and in every draw some row names some expert exactly 512 times.
All inputs are finite; a program needn't handle non-finite values.
Results may differ from the reference program's by a relative error of at most 0.015.
Values may be sent and summed in bfloat16 or wider, within the bound.
A program may use at most 320 MiB of HBM per device.

```python
import functools
import math
import jax
import jax.numpy as jnp
import numpy as np
from jax import lax

D = 1024
H = 16
KV = 8
HD = 64
FF = 512
TOPK = 8
SEQ = 512
SEGS = 8
ROWS = 32
TOKENS = 16384
EXPERTS = 16
CAP = 512


def shard_levels(key, shape, cuts, smallest, largest):
    loudness = 1.0
    for axis_at, parts in cuts:
        heights = jax.random.uniform(jax.random.fold_in(jax.random.fold_in(key, 6), axis_at), (parts,), jnp.float32, smallest / len(cuts), largest / len(cuts))
        loudness = loudness * jnp.repeat(jnp.exp(heights), shape[axis_at] // parts).reshape((-1,) + (1,) * (len(shape) - 1 - axis_at))
    return loudness


def split_up(number_of, total, bound, skew):
    weights = [(1 << 20) // math.isqrt(standing ** skew) + 1 for standing in range(2, number_of + 1)]
    spare, holding = total - bound - (number_of - 1), [1] * (number_of - 1)
    while spare > 0:
        candidates = [i for i in range(number_of - 1) if holding[i] < bound]
        whole, left = sum([weights[i] for i in candidates]), spare
        for i in candidates:
            addition = min(bound - holding[i], max(1, left * weights[i] // whole), spare)
            holding[i] = holding[i] + addition
            spare = spare - addition
    return np.array([bound] + holding)


def uneven_parts(key, number_of, total, bound, skew):
    if number_of == 2:
        one = jax.random.randint(key, (), max(1, total - bound), min(bound, total - 1) + 1)
        return jnp.stack([one, total - one])
    sizes = jnp.asarray(split_up(number_of, total, bound, skew), jnp.int32)
    pairs = (number_of - 1) // 2
    giver, taker = sizes[1:1 + 2 * pairs:2], sizes[2:2 + 2 * pairs:2]
    slack = jnp.minimum(giver - 1, bound - taker)
    moved = jax.random.randint(jax.random.fold_in(key, 1), (pairs,), 0, 1 << 20) % (slack + 1)
    sizes = sizes.at[1:1 + 2 * pairs:2].set(giver - moved).at[2:2 + 2 * pairs:2].set(taker + moved)
    return sizes[jax.random.permutation(jax.random.fold_in(key, 2), number_of)]


def deal_out(stream_key, own, number, rows, count, top, reach, skew):
    order = jax.random.permutation(stream_key, count)
    packed, ordinary = load_shares(count, rows * top, reach, skew, True), load_shares(count, rows * top, reach, skew, False)
    places = jnp.arange(count)

    def named(lengths, offset_by):
        used = int((lengths > 0).sum())
        fixed = max(1, used // 4)
        moved = fixed + (places - fixed + offset_by * (used - fixed)) % max(1, count - fixed)
        return jnp.zeros((count,), jnp.int32).at[order[jnp.where(places < fixed, places, moved)]].set(jnp.asarray(lengths, jnp.int32))

    lengths = jnp.where(number % 4 == 0, named(packed, number // 4), named(ordinary, number - number // 4 - 1))
    mixed = jax.random.permutation(jax.random.fold_in(own, 3), count)
    source_of, receiver = mixed[0:count // 2 * 2:2], mixed[1:count // 2 * 2:2]
    room = jnp.minimum(lengths[source_of] - 1, reach - lengths[receiver]) // 2
    room = jnp.where((source_of == order[0]) | (receiver == order[0]) | (lengths[receiver] == 0), 0, jnp.maximum(room, 0))
    moved = jax.random.randint(jax.random.fold_in(own, 4), (count // 2,), 0, 1 << 20) % (room + 1)
    lengths = lengths.at[source_of].add(-moved).at[receiver].add(moved)
    items = jnp.searchsorted(jnp.cumsum(lengths), jnp.arange(rows * top), side="right").astype(jnp.int32)
    grid = items.reshape(top, rows).T
    grid = grid[jax.random.permutation(jax.random.fold_in(own, 1), rows)]
    offset_by = jax.random.randint(jax.random.fold_in(own, 2), (rows, 1), 0, top)
    return jnp.take_along_axis(grid, (jnp.arange(top)[None, :] + offset_by) % top, axis=1)


def load_shares(number_of, total, bound, lean, full):
    loads = [(1 << 20) // math.isqrt(grade ** lean) + 1 for grade in range(1, number_of + 1)]
    largest = bound if full else min(bound, max(-(-total // number_of), total * loads[0] // sum(loads)))
    least = 1 if total - largest >= number_of - 1 else 0
    given, surplus = [largest] + [least] * (number_of - 1), total - largest - least * (number_of - 1)
    while surplus > 0:
        candidates = [i for i in range(1, number_of) if given[i] < largest] or [i for i in range(1, number_of) if given[i] < bound]
        whole, budget = sum([loads[i] for i in candidates]), surplus
        for i in candidates:
            addition = min(bound - given[i], max(1, budget * loads[i] // whole), surplus)
            given[i] = given[i] + addition
            surplus = surplus - addition
    return np.array(given)


def normal_values(own_key, shape, scale, limit, shards=(), held_as=jnp.bfloat16):
    entries = scale * jax.random.normal(own_key, shape, jnp.float32)
    if shards:
        entries = entries * shard_levels(own_key, shape, shards, -0.22, 0.18)
    return jnp.clip(entries, -limit, limit).astype(held_as)


def setup_inputs(seed: int = 0) -> dict:
    streams_of = jax.random.split(jax.random.key(seed), 15)
    hidden_in = normal_values(streams_of[0], (TOKENS, D), 1.0, 6.0, ((0, 32),))
    segment_ids = jax.vmap(lambda own: jnp.searchsorted(jnp.cumsum(uneven_parts(own, SEGS, SEQ, SEQ // 2, 2)), jnp.arange(SEQ), side="right"))(jax.random.split(streams_of[1], ROWS)).reshape((ROWS, SEQ)).astype(jnp.int32)
    expert_ids_keys = jax.random.split(jax.random.fold_in(streams_of[2], 1), TOKENS // SEQ)
    expert_ids_turns = jax.random.permutation(jax.random.fold_in(streams_of[2], 3), TOKENS // SEQ)
    expert_ids = jax.vmap(lambda own, number: deal_out(jax.random.fold_in(streams_of[2], 2), own, number, SEQ, EXPERTS, TOPK, CAP, 2))(expert_ids_keys, expert_ids_turns).reshape((TOKENS, TOPK))
    attn_gain = jnp.clip(1.0 + 0.1 * jax.random.normal(streams_of[3], (D,), jnp.float32), 0.5, 1.5)
    w_query = normal_values(streams_of[4], (D, H * HD), D ** -0.5, 0.1875)
    w_key = normal_values(streams_of[5], (D, KV * HD), D ** -0.5, 0.1875)
    w_value = normal_values(streams_of[6], (D, KV * HD), D ** -0.5, 0.1875)
    w_out = normal_values(streams_of[7], (H * HD, D), (H * HD // 16) ** -0.5, 0.75)
    ffn_gain = jnp.clip(1.0 + 0.1 * jax.random.normal(streams_of[8], (D,), jnp.float32), 0.5, 1.5)
    router = normal_values(streams_of[9], (D, EXPERTS), D ** -0.5, 0.1875)
    w_gate = normal_values(streams_of[10], (EXPERTS, D, FF), D ** -0.5, 0.1875, ((0, 16), (2, 2)))
    w_up = normal_values(streams_of[11], (EXPERTS, D, FF), D ** -0.5, 0.1875, ((0, 16), (2, 2)))
    w_down = normal_values(streams_of[12], (EXPERTS, FF, D), (FF // TOPK) ** -0.5, 0.75, ((0, 16), (1, 2)))
    grad_out = normal_values(streams_of[13], (TOKENS, D), 1.0, 6.0, ((0, 32),))
    return {"hidden_in": hidden_in, "segment_ids": segment_ids, "expert_ids": expert_ids, "attn_gain": attn_gain, "w_query": w_query, "w_key": w_key, "w_value": w_value, "w_out": w_out, "ffn_gain": ffn_gain, "router": router, "w_gate": w_gate, "w_up": w_up, "w_down": w_down, "grad_out": grad_out}


@jax.custom_vjp
def low(v):
    return lax.optimization_barrier(v.astype(jnp.bfloat16)).astype(jnp.float32)

@jax.custom_vjp
def low_back(v):
    return v

def low_keep(v):
    return (low(v), None)

def low_pass(kept, grad):
    return (grad,)

def back_keep(v):
    return (v, None)

def back_low(kept, grad):
    return (low(grad),)
low.defvjp(low_keep, low_pass)
low_back.defvjp(back_keep, back_low)
EPSILON = 1e-05
HIGH = lax.Precision.HIGHEST

def matmul_high(left, right):
    return jnp.dot(left, right, precision=HIGH)

def rms_norm(values, gain_vector):
    inv_rms = lax.rsqrt(lax.optimization_barrier(jnp.mean(values * values, axis=-1, keepdims=True)) + EPSILON)
    return values * inv_rms * gain_vector

def rope_tables(length, head_dim):
    half_size = head_dim // 2
    freqs = 10000.0 ** (-(jnp.arange(half_size, dtype=jnp.float32) * 2.0) / head_dim)
    angles = jnp.arange(length, dtype=jnp.float32)[:, None] * freqs[None, :]
    return (jnp.cos(angles), jnp.sin(angles))

def rotate(values, cosine_table, sine_table):
    half_size = values.shape[-1] // 2
    first_half = values[..., :half_size]
    second_half = values[..., half_size:]
    cosine_part = cosine_table[:, None, :]
    sine_part = sine_table[:, None, :]
    return jnp.concatenate([first_half * cosine_part - second_half * sine_part, second_half * cosine_part + first_half * sine_part], axis=-1)

def attend_row(row_block):
    query_rows, key_rows, value_rows, segments = row_block
    length = query_rows.shape[0]
    group_size = query_rows.shape[1] // key_rows.shape[1]
    grouped = query_rows.reshape(length, key_rows.shape[1], group_size, query_rows.shape[2])
    scores = jnp.einsum('qngd,knd->ngqk', grouped, key_rows, precision=HIGH) * query_rows.shape[2] ** (-0.5)
    places = jnp.arange(length, dtype=jnp.int32)
    allowed = (segments[:, None] == segments[None, :]) & (places[:, None] >= places[None, :])
    scores = low_back(jnp.where(allowed, scores, -1e+30))
    weights_prob = low(jax.nn.softmax(scores, axis=-1))
    attended = jnp.einsum('ngqk,knd->qngd', weights_prob, value_rows, precision=HIGH)
    return attended.reshape(length, -1)

def layer_forward(segment_ids, expert_ids, row_tables, hidden, attn_gain, w_query, w_key, w_value, w_out, ffn_gain, router, w_gate, w_up, w_down):
    tokens = hidden.shape[0]
    normed = low(rms_norm(hidden, attn_gain))
    query_pre = low_back(matmul_high(normed, w_query))
    key_pre = low_back(matmul_high(normed, w_key))
    value_rows = low(low_back(matmul_high(normed, w_value)))
    cosine_table, sine_table = rope_tables(SEQ, HD)
    query_rows = low(rotate(query_pre.reshape(ROWS, SEQ, H, HD), cosine_table, sine_table))
    key_rows = low(rotate(key_pre.reshape(ROWS, SEQ, KV, HD), cosine_table, sine_table))
    value_rows = value_rows.reshape(ROWS, SEQ, KV, HD)
    attended = lax.map(jax.checkpoint(attend_row), (query_rows, key_rows, value_rows, segment_ids))
    attended = low(low_back(attended.reshape(tokens, H * HD)))
    mixed_rows = hidden + low_back(matmul_high(attended, w_out))
    ffn_normed = low(rms_norm(mixed_rows, ffn_gain))
    logits = low_back(matmul_high(ffn_normed, router))
    chosen = jnp.take_along_axis(logits, expert_ids, axis=1)
    gate_probs = jax.nn.softmax(chosen, axis=-1)
    token_range = jnp.arange(tokens, dtype=jnp.int32)
    gate_table = jnp.zeros((tokens + 1, EXPERTS), jnp.float32).at[token_range[:, None], expert_ids].add(gate_probs)
    padded = jnp.concatenate([ffn_normed, jnp.zeros((1, D), jnp.float32)], axis=0)

    def expert_step(moe_total, expert_slab):
        gate_w, up_w, down_w, row_index, expert_index = expert_slab
        copies = low_back(padded[row_index])
        gate_act = low_back(matmul_high(copies, gate_w))
        up_act = low_back(matmul_high(copies, up_w))
        hidden_act = low(jax.nn.silu(gate_act) * up_act)
        outputs = low(low_back(matmul_high(hidden_act, down_w)))
        row_gates = gate_table[row_index, expert_index]
        return (moe_total.at[row_index].add(row_gates[:, None] * outputs), None)
    moe_total, unused = lax.scan(jax.checkpoint(expert_step), jnp.zeros((tokens + 1, D), jnp.float32), (w_gate, w_up, w_down, row_tables, jnp.arange(EXPERTS, dtype=jnp.int32)))
    return mixed_rows + moe_total[:tokens]

def reference(hidden_in, segment_ids, expert_ids, attn_gain, w_query, w_key, w_value, w_out, ffn_gain, router, w_gate, w_up, w_down, grad_out):
    tokens = hidden_in.shape[0]
    picked = expert_ids[:, :, None] == jnp.arange(EXPERTS, dtype=jnp.int32)[None, None, :]
    member = jnp.any(picked, axis=1)
    places = jnp.cumsum(member.astype(jnp.int32), axis=0) - 1
    places = jnp.where(member, places, ROWS * CAP).astype(jnp.int32)
    token_index = jnp.broadcast_to(jnp.arange(tokens, dtype=jnp.int32)[:, None], (tokens, EXPERTS))
    expert_index = jnp.broadcast_to(jnp.arange(EXPERTS, dtype=jnp.int32)[None, :], (tokens, EXPERTS))
    row_tables = jnp.full((EXPERTS, ROWS * CAP), tokens, jnp.int32).at[expert_index, places].set(token_index, mode='drop')
    floats = [item.astype(jnp.float32) for item in (hidden_in, attn_gain, w_query, w_key, w_value, w_out, ffn_gain, router, w_gate, w_up, w_down)]
    forward = functools.partial(layer_forward, segment_ids, expert_ids, row_tables)
    output, pullback = jax.vjp(forward, *floats)
    grads = pullback(grad_out.astype(jnp.float32))
    return (output.astype(jnp.bfloat16), grads[0].astype(jnp.bfloat16), grads[1], grads[2], grads[3], grads[4], grads[5], grads[6], grads[7], grads[8], grads[9], grads[10])
```

```python
import jax
import jax.numpy as jnp
from jax import lax
from jax.sharding import PartitionSpec as P

HD = 64


EPSILON = 1e-05


def norm_scale(values):
    return lax.rsqrt(jnp.mean(values * values, axis=-1, keepdims=True) + EPSILON)


def norm_back(values, inv_rms, gain_vector, grad_rows):
    weighted = grad_rows * gain_vector
    inner = jnp.mean(weighted * values, axis=-1, keepdims=True)
    value_grad = inv_rms * weighted - values * (inv_rms * inv_rms * inv_rms) * inner
    return (value_grad, jnp.sum(grad_rows * values * inv_rms, axis=0))


def rope_tables(length, head_dim):
    half_size = head_dim // 2
    freqs = 10000.0 ** (-(jnp.arange(half_size, dtype=jnp.float32) * 2.0) / head_dim)
    angles = jnp.arange(length, dtype=jnp.float32)[:, None] * freqs[None, :]
    return (jnp.cos(angles), jnp.sin(angles))


def rotate(values, cosine_table, sine_table, direction):
    half_size = values.shape[-1] // 2
    first_half = values[..., :half_size]
    second_half = values[..., half_size:]
    cosine_part = cosine_table[:, None, :]
    sine_part = sine_table[:, None, :] * direction
    return jnp.concatenate(
        [
            first_half * cosine_part - second_half * sine_part,
            second_half * cosine_part + first_half * sine_part,
        ],
        axis=-1,
    )


def attention_probs(grouped, key_rows, allowed, head_dim):
    scores = jnp.einsum(
        "qngd,knd->ngqk", grouped, key_rows, preferred_element_type=jnp.float32
    ) * head_dim ** (-0.5)
    return jnp.where(allowed, scores, -1e30)


def on_device(
    hidden_in,
    segment_ids,
    expert_ids,
    attn_gain,
    w_query,
    w_key,
    w_value,
    w_out,
    ffn_gain,
    router,
    w_gate,
    w_up,
    w_down,
    grad_out,
):
    f32 = jnp.float32
    bf16 = jnp.bfloat16
    length, model_width = hidden_in.shape
    head_dim = HD
    head_count = w_query.shape[1] // head_dim
    kv_count = w_key.shape[1] // head_dim
    group_size = head_count // kv_count
    experts = router.shape[1]
    rows_grad = lax.all_gather(grad_out, "wide", axis=0, tiled=True)
    full_gate, full_up, full_down = (
        lax.all_gather(w_gate, "narrow", axis=2, tiled=True),
        lax.all_gather(w_up, "narrow", axis=2, tiled=True),
        lax.all_gather(w_down, "narrow", axis=1, tiled=True),
    )
    inputs = hidden_in.astype(f32)
    scale_one = norm_scale(inputs)
    normed = (inputs * scale_one * attn_gain).astype(bf16)
    query_pre = jnp.dot(normed, w_query, preferred_element_type=f32)
    key_pre = jnp.dot(normed, w_key, preferred_element_type=f32)
    value_pre = jnp.dot(normed, w_value, preferred_element_type=f32)
    cosine_table, sine_table = rope_tables(length, head_dim)
    query_rows = rotate(
        query_pre.reshape(length, head_count, head_dim), cosine_table, sine_table, 1.0
    ).astype(bf16)
    key_rows = rotate(
        key_pre.reshape(length, kv_count, head_dim), cosine_table, sine_table, 1.0
    ).astype(bf16)
    value_rows = value_pre.astype(bf16).reshape(length, kv_count, head_dim)
    grouped = query_rows.reshape(length, kv_count, group_size, head_dim)
    segments = segment_ids[0]
    places = jnp.arange(length, dtype=jnp.int32)
    allowed = (segments[:, None] == segments[None, :]) & (places[:, None] >= places[None, :])
    scores = attention_probs(grouped, key_rows, allowed, head_dim)
    row_max = jnp.max(scores, axis=-1, keepdims=True)
    log_total = row_max + jnp.log(jnp.sum(jnp.exp(scores - row_max), axis=-1, keepdims=True))
    weights_prob = jnp.exp(scores - log_total)
    attended = jnp.einsum(
        "ngqk,knd->qngd", weights_prob.astype(bf16), value_rows, preferred_element_type=f32
    )
    attended = attended.reshape(length, head_count * head_dim).astype(bf16)
    mixed_rows = inputs + jnp.dot(attended, w_out, preferred_element_type=f32)
    scale_two = norm_scale(mixed_rows)
    ffn_normed = (mixed_rows * scale_two * ffn_gain).astype(bf16)
    logits = jnp.dot(ffn_normed, router, preferred_element_type=f32)
    picked = expert_ids[:, :, None] == jnp.arange(experts, dtype=jnp.int32)[None, None, :]
    member = jnp.any(picked, axis=1)
    masked = jnp.where(member, logits, -jnp.inf)
    powers = jnp.where(member, jnp.exp(masked - jnp.max(masked, axis=-1, keepdims=True)), 0.0)
    gate_probs = powers / jnp.sum(powers, axis=-1, keepdims=True)
    row_gates = lax.all_to_all(gate_probs.T, "wide", split_axis=0, concat_axis=0, tiled=True)
    row_gates = row_gates.reshape(-1, 1)
    rows_in = lax.all_gather(ffn_normed, "wide", axis=0, tiled=True)
    gate_act = jnp.dot(rows_in, full_gate[0], preferred_element_type=f32)
    up_act = jnp.dot(rows_in, full_up[0], preferred_element_type=f32)
    hidden_act = (jax.nn.silu(gate_act) * up_act).astype(bf16)
    outputs = jnp.dot(hidden_act, full_down[0], preferred_element_type=f32).astype(bf16)
    moe_rows = lax.psum_scatter(
        (row_gates * outputs.astype(f32)).astype(bf16), "wide", scatter_dimension=0, tiled=True
    )
    hidden_out = (mixed_rows + moe_rows.astype(f32)).astype(bf16)
    cotangent = grad_out.astype(f32)
    gate_dots = jnp.sum(outputs.astype(f32) * rows_grad.astype(f32), axis=-1)
    gate_grads = lax.all_to_all(
        gate_dots.reshape(experts, length), "wide", split_axis=0, concat_axis=0, tiled=True
    ).T
    logit_grads = (
        gate_probs * (gate_grads - jnp.sum(gate_probs * gate_grads, axis=-1, keepdims=True))
    ).astype(bf16)
    router_grad = jnp.einsum("sd,se->de", ffn_normed, logit_grads, preferred_element_type=f32)
    normed_two_grad = jnp.einsum("se,de->sd", logit_grads, router, preferred_element_type=f32)
    grads_in = (row_gates * rows_grad.astype(f32)).astype(bf16)
    hidden_grad = jnp.einsum("rd,fd->rf", grads_in, full_down[0], preferred_element_type=f32)
    down_w_grad = jnp.einsum("rf,rd->fd", hidden_act, grads_in, preferred_element_type=f32)
    sigmoid_gate = jax.nn.sigmoid(gate_act)
    gate_grad = (
        hidden_grad * up_act * sigmoid_gate * (1.0 + gate_act * (1.0 - sigmoid_gate))
    ).astype(bf16)
    up_grad = (hidden_grad * gate_act * sigmoid_gate).astype(bf16)
    gate_w_grad = jnp.einsum("rd,rf->df", rows_in, gate_grad, preferred_element_type=f32)
    up_w_grad = jnp.einsum("rd,rf->df", rows_in, up_grad, preferred_element_type=f32)
    copy_grads = (
        jnp.einsum("rf,df->rd", gate_grad, full_gate[0], preferred_element_type=f32)
        + jnp.einsum("rf,df->rd", up_grad, full_up[0], preferred_element_type=f32)
    ).astype(bf16)
    rows_back = lax.psum_scatter(copy_grads, "wide", scatter_dimension=0, tiled=True)
    gate_w_grad, up_w_grad, down_w_grad = (
        lax.psum_scatter(
            gate_w_grad[None].astype(jnp.bfloat16), "narrow", scatter_dimension=2, tiled=True
        ).astype(jnp.float32),
        lax.psum_scatter(
            up_w_grad[None].astype(jnp.bfloat16), "narrow", scatter_dimension=2, tiled=True
        ).astype(jnp.float32),
        lax.psum_scatter(
            down_w_grad[None].astype(jnp.bfloat16), "narrow", scatter_dimension=1, tiled=True
        ).astype(jnp.float32),
    )
    normed_two_grad = normed_two_grad + rows_back.astype(f32)
    mixed_part, ffn_gain_grad = norm_back(mixed_rows, scale_two, ffn_gain, normed_two_grad)
    mixed_grad = cotangent + mixed_part
    branch_grad = mixed_grad.astype(bf16)
    out_w_grad = jnp.einsum("sh,sd->hd", attended, branch_grad, preferred_element_type=f32)
    attended_grad = jnp.einsum("sd,hd->sh", branch_grad, w_out, preferred_element_type=f32).astype(
        bf16
    )
    attended_grad = attended_grad.reshape(length, kv_count, group_size, head_dim)
    scores = attention_probs(grouped, key_rows, allowed, head_dim)
    weights_prob = jnp.exp(scores - log_total)
    value_grad = jnp.einsum(
        "ngqk,qngd->knd", weights_prob.astype(bf16), attended_grad, preferred_element_type=f32
    )
    prob_grad = jnp.einsum("qngd,knd->ngqk", attended_grad, value_rows, preferred_element_type=f32)
    score_grad = (
        weights_prob * (prob_grad - jnp.sum(weights_prob * prob_grad, axis=-1, keepdims=True))
    ).astype(bf16)
    query_grad = jnp.einsum(
        "ngqk,knd->qngd", score_grad, key_rows, preferred_element_type=f32
    ) * head_dim ** (-0.5)
    key_grad = jnp.einsum(
        "ngqk,qngd->knd", score_grad, grouped, preferred_element_type=f32
    ) * head_dim ** (-0.5)
    query_grad = rotate(
        query_grad.reshape(length, head_count, head_dim), cosine_table, sine_table, -1.0
    )
    query_grad = query_grad.reshape(length, -1).astype(bf16)
    key_grad = rotate(key_grad, cosine_table, sine_table, -1.0).reshape(length, -1).astype(bf16)
    value_grad = value_grad.reshape(length, -1).astype(bf16)
    query_w_grad = jnp.einsum("sd,sh->dh", normed, query_grad, preferred_element_type=f32)
    key_w_grad = jnp.einsum("sd,sh->dh", normed, key_grad, preferred_element_type=f32)
    value_w_grad = jnp.einsum("sd,sh->dh", normed, value_grad, preferred_element_type=f32)
    normed_one_grad = (
        jnp.einsum("sh,dh->sd", query_grad, w_query, preferred_element_type=f32)
        + jnp.einsum("sh,dh->sd", key_grad, w_key, preferred_element_type=f32)
        + jnp.einsum("sh,dh->sd", value_grad, w_value, preferred_element_type=f32)
    )
    input_part, attn_gain_grad = norm_back(inputs, scale_one, attn_gain, normed_one_grad)
    grad_in = (mixed_grad + input_part).astype(bf16)
    small = jnp.concatenate(
        [
            attn_gain_grad.reshape(-1, 128),
            ffn_gain_grad.reshape(-1, 128),
            router_grad.reshape(-1, 128),
        ],
        axis=0,
    )
    everywhere = ("wide", "narrow")
    columns = jnp.concatenate([query_w_grad, key_w_grad, value_w_grad, out_w_grad], axis=1)
    shares = lax.psum_scatter(columns.astype(bf16), everywhere, scatter_dimension=0, tiled=True)
    columns = lax.all_gather(shares, everywhere, axis=0, tiled=True).astype(f32)
    small = lax.psum(small, everywhere)
    gain_rows = model_width // 128
    query_width, key_width = w_query.shape[1], w_key.shape[1]
    summed = (
        small[:gain_rows].reshape(-1),
        columns[:, :query_width],
        columns[:, query_width : query_width + key_width],
        columns[:, query_width + key_width : query_width + 2 * key_width],
        columns[:, query_width + 2 * key_width :],
        small[gain_rows : 2 * gain_rows].reshape(-1),
        small[2 * gain_rows :].reshape(router.shape),
    )
    return (
        hidden_out,
        grad_in,
        summed[0],
        summed[1],
        summed[2],
        summed[3],
        summed[4],
        summed[5],
        summed[6],
        gate_w_grad,
        up_w_grad,
        down_w_grad,
    )


def solution(mesh):
    return jax.shard_map(
        on_device,
        mesh=mesh,
        in_specs=(
            P(("wide", "narrow"), None),
            P(("wide", "narrow"), None),
            P(("wide", "narrow"), None),
            P(),
            P(),
            P(),
            P(),
            P(),
            P(),
            P(),
            P("wide", None, "narrow"),
            P("wide", None, "narrow"),
            P("wide", "narrow", None),
            P(("wide", "narrow"), None),
        ),
        out_specs=(
            P(("wide", "narrow"), None),
            P(("wide", "narrow"), None),
            P(),
            P(),
            P(),
            P(),
            P(),
            P(),
            P(),
            P("wide", None, "narrow"),
            P("wide", None, "narrow"),
            P("wide", "narrow", None),
        ),
        check_vma=False,
    )
```

```python
import jax
import jax.numpy as jnp
from jax import lax
from jax.sharding import Mesh
from jax.sharding import PartitionSpec as P

HD = 64
INNER = 4


EPSILON = 1e-05


def norm_scale(values):
    return lax.rsqrt(jnp.mean(values * values, axis=-1, keepdims=True) + EPSILON)


def norm_back(values, inv_rms, gain_vector, grad_rows):
    weighted = grad_rows * gain_vector
    inner = jnp.mean(weighted * values, axis=-1, keepdims=True)
    value_grad = inv_rms * weighted - values * (inv_rms * inv_rms * inv_rms) * inner
    return (value_grad, jnp.sum(grad_rows * values * inv_rms, axis=0))


def rope_tables(length, head_dim):
    half_size = head_dim // 2
    freqs = 10000.0 ** (-(jnp.arange(half_size, dtype=jnp.float32) * 2.0) / head_dim)
    angles = jnp.arange(length, dtype=jnp.float32)[:, None] * freqs[None, :]
    return (jnp.cos(angles), jnp.sin(angles))


def rotate(values, cosine_table, sine_table, direction):
    half_size = values.shape[-1] // 2
    first_half = values[..., :half_size]
    second_half = values[..., half_size:]
    cosine_part = cosine_table[:, None, :]
    sine_part = sine_table[:, None, :] * direction
    return jnp.concatenate(
        [
            first_half * cosine_part - second_half * sine_part,
            second_half * cosine_part + first_half * sine_part,
        ],
        axis=-1,
    )


def attention_probs(grouped, key_rows, allowed, head_dim):
    scores = jnp.einsum(
        "qngd,knd->ngqk", grouped, key_rows, preferred_element_type=jnp.float32
    ) * head_dim ** (-0.5)
    return jnp.where(allowed, scores, -1e30)


def on_device(
    hidden_in,
    segment_ids,
    expert_ids,
    attn_gain,
    w_query,
    w_key,
    w_value,
    w_out,
    ffn_gain,
    router,
    w_gate,
    w_up,
    w_down,
    grad_out,
):
    f32 = jnp.float32
    bf16 = jnp.bfloat16
    length, model_width = hidden_in.shape
    head_dim = HD
    head_count = w_query.shape[1] // head_dim
    kv_count = w_key.shape[1] // head_dim
    group_size = head_count // kv_count
    experts = router.shape[1]
    outer_count = experts // INNER
    here = ("inner", "narrow")
    full_gate = lax.all_gather(w_gate[0], "outer", axis=1, tiled=True)
    full_up = lax.all_gather(w_up[0], "outer", axis=1, tiled=True)
    full_down = lax.all_gather(w_down[0], "outer", axis=0, tiled=True)
    rows_grad = lax.all_gather(grad_out, here, axis=0, tiled=True)
    part = w_gate.shape[2]
    inputs = hidden_in.astype(f32)
    scale_one = norm_scale(inputs)
    normed = (inputs * scale_one * attn_gain).astype(bf16)
    query_pre = jnp.dot(normed, w_query, preferred_element_type=f32)
    key_pre = jnp.dot(normed, w_key, preferred_element_type=f32)
    value_pre = jnp.dot(normed, w_value, preferred_element_type=f32)
    cosine_table, sine_table = rope_tables(length, head_dim)
    query_rows = rotate(
        query_pre.reshape(length, head_count, head_dim), cosine_table, sine_table, 1.0
    ).astype(bf16)
    key_rows = rotate(
        key_pre.reshape(length, kv_count, head_dim), cosine_table, sine_table, 1.0
    ).astype(bf16)
    value_rows = value_pre.astype(bf16).reshape(length, kv_count, head_dim)
    grouped = query_rows.reshape(length, kv_count, group_size, head_dim)
    segments = segment_ids[0]
    places = jnp.arange(length, dtype=jnp.int32)
    allowed = (segments[:, None] == segments[None, :]) & (places[:, None] >= places[None, :])
    scores = attention_probs(grouped, key_rows, allowed, head_dim)
    row_max = jnp.max(scores, axis=-1, keepdims=True)
    log_total = row_max + jnp.log(jnp.sum(jnp.exp(scores - row_max), axis=-1, keepdims=True))
    weights_prob = jnp.exp(scores - log_total)
    attended = jnp.einsum(
        "ngqk,knd->qngd", weights_prob.astype(bf16), value_rows, preferred_element_type=f32
    )
    attended = attended.reshape(length, head_count * head_dim).astype(bf16)
    mixed_rows = inputs + jnp.dot(attended, w_out, preferred_element_type=f32)
    scale_two = norm_scale(mixed_rows)
    ffn_normed = (mixed_rows * scale_two * ffn_gain).astype(bf16)
    logits = jnp.dot(ffn_normed, router, preferred_element_type=f32)
    picked = expert_ids[:, :, None] == jnp.arange(experts, dtype=jnp.int32)[None, None, :]
    member = jnp.any(picked, axis=1)
    masked = jnp.where(member, logits, -jnp.inf)
    powers = jnp.where(member, jnp.exp(masked - jnp.max(masked, axis=-1, keepdims=True)), 0.0)
    gate_probs = powers / jnp.sum(powers, axis=-1, keepdims=True)
    gate_table = lax.all_gather(gate_probs.T, here, axis=0, tiled=False)
    gate_table = gate_table.reshape(-1, outer_count, INNER, length)
    mine = lax.dynamic_index_in_dim(gate_table, lax.axis_index("inner"), 2, keepdims=False)
    row_gates = mine.transpose(0, 2, 1).reshape(-1, outer_count)
    gate_wide = jnp.repeat(row_gates, part, axis=1)
    rows_in = lax.all_gather(ffn_normed, here, axis=0, tiled=True)
    gate_act = jnp.dot(rows_in, full_gate, preferred_element_type=f32)
    up_act = jnp.dot(rows_in, full_up, preferred_element_type=f32)
    raw_grad = jnp.einsum("rd,fd->rf", rows_grad, full_down, preferred_element_type=f32)
    sigmoid_gate = jax.nn.sigmoid(gate_act)
    plain_act = gate_act * sigmoid_gate * up_act
    hidden_act = (gate_wide * plain_act).astype(bf16)
    hidden_grad = gate_wide * raw_grad
    moe_rows = lax.psum_scatter(
        jnp.dot(hidden_act, full_down, preferred_element_type=f32).astype(bf16),
        here,
        scatter_dimension=0,
        tiled=True,
    )
    hidden_out = (mixed_rows + moe_rows.astype(f32)).astype(bf16)
    cotangent = grad_out.astype(f32)
    gate_dots = jnp.sum((plain_act * raw_grad).reshape(-1, outer_count, part), axis=-1)
    lane = jnp.arange(INNER) == lax.axis_index("inner")
    gate_dots = jnp.where(lane[None, None, :], gate_dots[:, :, None], 0.0).reshape(-1, experts)
    gate_grads = lax.psum_scatter(gate_dots, here, scatter_dimension=0, tiled=True)
    logit_grads = (
        gate_probs * (gate_grads - jnp.sum(gate_probs * gate_grads, axis=-1, keepdims=True))
    ).astype(bf16)
    router_grad = jnp.einsum("sd,se->de", ffn_normed, logit_grads, preferred_element_type=f32)
    normed_two_grad = jnp.einsum("se,de->sd", logit_grads, router, preferred_element_type=f32)
    gate_grad = (
        hidden_grad * up_act * sigmoid_gate * (1.0 + gate_act * (1.0 - sigmoid_gate))
    ).astype(bf16)
    up_grad = (hidden_grad * gate_act * sigmoid_gate).astype(bf16)
    copy_grads = (
        jnp.einsum("rf,df->rd", gate_grad, full_gate, preferred_element_type=f32)
        + jnp.einsum("rf,df->rd", up_grad, full_up, preferred_element_type=f32)
    ).astype(bf16)
    rows_back = lax.psum_scatter(copy_grads, here, scatter_dimension=0, tiled=True)
    down_w_grad = jnp.einsum("rf,rd->fd", hidden_act, rows_grad, preferred_element_type=f32)
    gate_w_grad = jnp.einsum("rd,rf->df", rows_in, gate_grad, preferred_element_type=f32)
    up_w_grad = jnp.einsum("rd,rf->df", rows_in, up_grad, preferred_element_type=f32)
    gate_w_grad, up_w_grad, down_w_grad = (
        lax.psum_scatter(gate_w_grad.astype(bf16), "outer", scatter_dimension=1, tiled=True),
        lax.psum_scatter(up_w_grad.astype(bf16), "outer", scatter_dimension=1, tiled=True),
        lax.psum_scatter(down_w_grad.astype(bf16), "outer", scatter_dimension=0, tiled=True),
    )
    gate_w_grad, up_w_grad, down_w_grad = (
        gate_w_grad[None].astype(f32),
        up_w_grad[None].astype(f32),
        down_w_grad[None].astype(f32),
    )
    normed_two_grad = normed_two_grad + rows_back.astype(f32)
    mixed_part, ffn_gain_grad = norm_back(mixed_rows, scale_two, ffn_gain, normed_two_grad)
    mixed_grad = cotangent + mixed_part
    branch_grad = mixed_grad.astype(bf16)
    out_w_grad = jnp.einsum("sh,sd->hd", attended, branch_grad, preferred_element_type=f32)
    attended_grad = jnp.einsum("sd,hd->sh", branch_grad, w_out, preferred_element_type=f32).astype(
        bf16
    )
    attended_grad = attended_grad.reshape(length, kv_count, group_size, head_dim)
    scores = attention_probs(grouped, key_rows, allowed, head_dim)
    weights_prob = jnp.exp(scores - log_total)
    value_grad = jnp.einsum(
        "ngqk,qngd->knd", weights_prob.astype(bf16), attended_grad, preferred_element_type=f32
    )
    prob_grad = jnp.einsum("qngd,knd->ngqk", attended_grad, value_rows, preferred_element_type=f32)
    score_grad = (
        weights_prob * (prob_grad - jnp.sum(weights_prob * prob_grad, axis=-1, keepdims=True))
    ).astype(bf16)
    query_grad = jnp.einsum(
        "ngqk,knd->qngd", score_grad, key_rows, preferred_element_type=f32
    ) * head_dim ** (-0.5)
    key_grad = jnp.einsum(
        "ngqk,qngd->knd", score_grad, grouped, preferred_element_type=f32
    ) * head_dim ** (-0.5)
    query_grad = rotate(
        query_grad.reshape(length, head_count, head_dim), cosine_table, sine_table, -1.0
    )
    query_grad = query_grad.reshape(length, -1).astype(bf16)
    key_grad = rotate(key_grad, cosine_table, sine_table, -1.0).reshape(length, -1).astype(bf16)
    value_grad = value_grad.reshape(length, -1).astype(bf16)
    query_w_grad = jnp.einsum("sd,sh->dh", normed, query_grad, preferred_element_type=f32)
    key_w_grad = jnp.einsum("sd,sh->dh", normed, key_grad, preferred_element_type=f32)
    value_w_grad = jnp.einsum("sd,sh->dh", normed, value_grad, preferred_element_type=f32)
    normed_one_grad = (
        jnp.einsum("sh,dh->sd", query_grad, w_query, preferred_element_type=f32)
        + jnp.einsum("sh,dh->sd", key_grad, w_key, preferred_element_type=f32)
        + jnp.einsum("sh,dh->sd", value_grad, w_value, preferred_element_type=f32)
    )
    input_part, attn_gain_grad = norm_back(inputs, scale_one, attn_gain, normed_one_grad)
    grad_in = (mixed_grad + input_part).astype(bf16)
    everywhere = ("outer", "inner", "narrow")
    small = jnp.concatenate(
        [router_grad, attn_gain_grad[:, None], ffn_gain_grad[:, None]], axis=1
    )
    small = jnp.pad(small, ((0, 0), (0, 128 - small.shape[1])))
    columns = jnp.concatenate(
        [query_w_grad, key_w_grad, value_w_grad, out_w_grad, small], axis=1
    )
    shares = lax.psum_scatter(columns.astype(bf16), everywhere, scatter_dimension=0, tiled=True)
    columns = lax.all_gather(shares, everywhere, axis=0, tiled=True).astype(f32)
    starts = [0]
    for width in (w_query.shape[1], w_key.shape[1], w_value.shape[1], model_width, experts, 1, 1):
        starts.append(starts[-1] + width)
    pieces = [columns[:, low:high] for low, high in zip(starts[:-1], starts[1:])]
    summed = (
        pieces[5][:, 0],
        pieces[0],
        pieces[1],
        pieces[2],
        pieces[3],
        pieces[6][:, 0],
        pieces[4],
    )
    return (
        hidden_out,
        grad_in,
        summed[0],
        summed[1],
        summed[2],
        summed[3],
        summed[4],
        summed[5],
        summed[6],
        gate_w_grad,
        up_w_grad,
        down_w_grad,
    )


def solution(mesh):
    names = ("outer", "inner", "narrow")
    narrow = mesh.shape["narrow"]
    cut = Mesh(mesh.devices.reshape(-1, INNER, narrow), names)
    rows = P(names, None)
    columns = P(("outer", "inner"), None, "narrow")
    depths = P(("outer", "inner"), "narrow", None)
    return jax.shard_map(
        on_device,
        mesh=cut,
        in_specs=(rows, rows, rows) + (P(),) * 7 + (columns, columns, depths, rows),
        out_specs=(rows, rows) + (P(),) * 7 + (columns, columns, depths),
        check_vma=False,
    )
```

```python
import functools

import jax
import jax.numpy as jnp
from jax import lax
from jax.experimental import pallas as pl
from jax.experimental.pallas import tpu as pltpu
from jax.sharding import Mesh
from jax.sharding import PartitionSpec as P

HD = 64
INNER = 4


EPSILON = 1e-05


def norm_scale(values):
    return lax.rsqrt(jnp.mean(values * values, axis=-1, keepdims=True) + EPSILON)


def norm_back(values, inv_rms, gain_vector, grad_rows):
    weighted = grad_rows * gain_vector
    inner = jnp.mean(weighted * values, axis=-1, keepdims=True)
    value_grad = inv_rms * weighted - values * (inv_rms * inv_rms * inv_rms) * inner
    return (value_grad, jnp.sum(grad_rows * values * inv_rms, axis=0))


def rope_tables(length, head_dim):
    half_size = head_dim // 2
    freqs = 10000.0 ** (-(jnp.arange(half_size, dtype=jnp.float32) * 2.0) / head_dim)
    angles = jnp.arange(length, dtype=jnp.float32)[:, None] * freqs[None, :]
    return (jnp.cos(angles), jnp.sin(angles))


def rotate(values, cosine_table, sine_table, direction):
    half_size = values.shape[-1] // 2
    first_half = values[..., :half_size]
    second_half = values[..., half_size:]
    cosine_part = cosine_table[:, None, :]
    sine_part = sine_table[:, None, :] * direction
    return jnp.concatenate(
        [
            first_half * cosine_part - second_half * sine_part,
            second_half * cosine_part + first_half * sine_part,
        ],
        axis=-1,
    )


def attention_probs(grouped, key_rows, allowed, head_dim):
    scores = jnp.einsum(
        "qngd,knd->ngqk", grouped, key_rows, preferred_element_type=jnp.float32
    ) * head_dim ** (-0.5)
    return jnp.where(allowed, scores, -1e30)


def dot_nn(left, right):
    return lax.dot_general(left, right, (((1,), (0,)), ((), ())), preferred_element_type=jnp.float32)


def dot_nt(left, right):
    return lax.dot_general(left, right, (((1,), (1,)), ((), ())), preferred_element_type=jnp.float32)


def dot_tn(left, right):
    return lax.dot_general(left, right, (((0,), (0,)), ((), ())), preferred_element_type=jnp.float32)


def expert_kernel(
    outer_count,
    x_hbm,
    gate_hbm,
    grad_hbm,
    pair_own,
    down_own,
    pair_next,
    down_next,
    dx_hbm,
    y_hbm,
    dots_ref,
    first_hbm,
    last_hbm,
    rows,
    gates,
    act,
    both,
    wide,
    down,
    grads,
    total,
    stage_a,
    stage_b,
    ring,
    core_in,
    relay_in,
    last_in,
    dots,
    dots_in,
    local_sem,
    grad_sem,
    y_sem,
    gather_send,
    gather_recv,
    weight_send,
    weight_recv,
    ring_send,
    ring_recv,
    dots_send,
    dots_recv,
    back_send,
    back_recv,
):
    f32 = jnp.float32
    bf16 = jnp.bfloat16
    length, part = rows.shape[1], down.shape[1]
    half = length // 2
    outer, inner, narrow = lax.axis_index("outer"), lax.axis_index("inner"), lax.axis_index("narrow")
    side, core = inner // 2, inner % 2
    core_at = {"inner": side * 2 + (1 - core)}
    x_at = {"narrow": 1 - narrow}
    y_at = {"inner": (1 - side) * 2 + core}
    next_at = {"outer": lax.rem(outer + 1, outer_count)}
    before_at = {"outer": lax.rem(outer + outer_count - 1, outer_count)}

    def device_of(slot):
        there = slot // 2
        return {
            "inner": ((side + there // 2) % 2) * 2 + (core + slot % 2) % 2,
            "narrow": (narrow + there % 2) % 2,
        }

    def place_of(slot):
        there = slot // 2
        at_inner = ((side + there // 2) % 2) * 2 + (core + slot % 2) % 2
        return at_inner * 2 + (narrow + there % 2) % 2

    def remote(source, target, sends, recvs, index, device):
        return pltpu.make_async_remote_copy(
            src_ref=source,
            dst_ref=target,
            send_sem=sends.at[index],
            recv_sem=recvs.at[index],
            device_id=device,
            device_id_type=pl.DeviceIdType.MESH,
        )

    def local(source, target, index):
        return pltpu.make_async_copy(source, target, local_sem.at[index])

    low, high = pl.ds(0, half), pl.ds(half, half)
    dx_ref = total.at[pl.ds(0, length)]

    def gather(index):
        source, target, device = (
            (rows.at[0], rows.at[1], core_at),
            (rows.at[0], rows.at[2], x_at),
            (rows.at[0], rows.at[4], y_at),
            (rows.at[2, low], rows.at[6, low], y_at),
            (rows.at[4, high], rows.at[6, high], x_at),
            (rows.at[2], rows.at[3], core_at),
            (rows.at[4], rows.at[5], core_at),
            (rows.at[6], rows.at[7], core_at),
            (gates.at[0], gates.at[1], core_at),
            (gates.at[0], gates.at[2], x_at),
            (gates.at[0], gates.at[4], y_at),
            (gates.at[0], gates.at[6], device_of(6)),
            (gates.at[2], gates.at[3], core_at),
            (gates.at[4], gates.at[5], core_at),
            (gates.at[6], gates.at[7], core_at),
        )[index]
        return remote(source, target, gather_send, gather_recv, index, device)

    def wide_at(slot):
        return wide.at[:, pl.ds(slot * 2 * part, 2 * part)]

    def weight(index):
        slot = 1 + index // 2
        if index % 2 == 0:
            return remote(
                wide_at(slot), wide_at(slot + 1), weight_send, weight_recv, index, next_at
            )
        return remote(
            down.at[slot], down.at[slot + 1], weight_send, weight_recv, index, next_at
        )

    def ring_copy(index):
        source = (stage_a, stage_b)[index]
        return remote(source, ring.at[index], ring_send, ring_recv, index, next_at)

    def dots_copy(slot):
        return remote(
            dots.at[slot], dots_in.at[slot], dots_send, dots_recv, slot, device_of(slot)
        )

    def back(index):
        source, target, device = (
            (rows.at[1], core_in.at[0], core_at),
            (rows.at[3], core_in.at[1], core_at),
            (rows.at[5], core_in.at[2], core_at),
            (rows.at[7], core_in.at[3], core_at),
            (rows.at[6, low], relay_in.at[0], x_at),
            (rows.at[6, high], relay_in.at[1], y_at),
            (rows.at[2], last_in.at[0], x_at),
            (rows.at[4], last_in.at[1], y_at),
        )[index]
        return remote(source, target, back_send, back_recv, index, device)

    own_copies = (
        local(x_hbm, rows.at[0], 0),
        local(gate_hbm, gates.at[0], 1),
        local(pair_next, wide_at(1), 2),
        local(down_next, down.at[1], 3),
        local(pair_own, wide_at(0), 4),
        local(down_own, down.at[0], 5),
    )
    for copy in own_copies:
        copy.start()

    def fetch(step):
        order = step % 8
        slot = jnp.where(order == 3, 4, jnp.where(order == 4, 3, order))
        return pltpu.make_async_copy(
            grad_hbm.at[place_of(slot)], grads.at[step % 2], grad_sem.at[step % 2]
        )

    fetch(0).start()
    barrier = pltpu.get_barrier_semaphore()
    for slot in range(1, 8):
        pl.semaphore_signal(
            barrier, inc=1, device_id=device_of(slot), device_id_type=pl.DeviceIdType.MESH
        )
    for device in (next_at, before_at):
        pl.semaphore_signal(
            barrier, inc=1, device_id=device, device_id_type=pl.DeviceIdType.MESH
        )
    pl.semaphore_wait(barrier, 9)
    own_copies[0].wait()
    own_copies[1].wait()
    for index in (1, 2, 9, 10, 11, 0, 8):
        gather(index).start()
    for copy in own_copies[2:]:
        copy.wait()
    weight(0).start()
    weight(1).start()

    def first_step(step, carry):
        turn, order = step // 8, step % 8
        slot = jnp.where(order == 3, 4, jnp.where(order == 4, 3, order))
        block = jnp.where(turn == 0, 1, jnp.where(turn == 1, 2, jnp.where(turn == 2, 0, 3)))

        @pl.when(step + 1 < 8 * outer_count)
        def _():
            fetch(step + 1).start()

        @pl.when(step == 1)
        def _():
            gather(0).wait_recv()
            gather(8).wait_recv()

        @pl.when(step == 2)
        def _():
            gather(1).wait_recv()
            gather(3).start()
            gather(5).start()
            gather(2).wait_recv()
            gather(4).start()
            gather(6).start()
            gather(9).wait_recv()
            gather(12).start()
            gather(10).wait_recv()
            gather(13).start()

        @pl.when(step == 4)
        def _():
            gather(5).wait_recv()
            gather(12).wait_recv()

        @pl.when(step == 5)
        def _():
            gather(6).wait_recv()
            gather(13).wait_recv()

        @pl.when(step == 6)
        def _():
            gather(3).wait_recv()
            gather(4).wait_recv()
            gather(7).start()
            gather(11).wait_recv()
            gather(14).start()

        @pl.when(step == 7)
        def _():
            gather(7).wait_recv()
            gather(14).wait_recv()

        @pl.when(step == 8)
        def _():
            weight(0).wait_recv()
            weight(1).wait_recv()
            weight(2).start()
            weight(3).start()

        @pl.when(step == 24)
        def _():
            weight(2).wait_recv()
            weight(3).wait_recv()

        fetch(step).wait()
        here = rows[slot]
        grad_rows = grads[step % 2]
        products = dot_nn(here, wide[:, pl.ds(block * 2 * part, 2 * part)])
        gate_act, up_act = products[:, :part], products[:, part:]
        raw = dot_nt(grad_rows, down[block])
        expert = lax.rem(outer + outer_count - block, outer_count) * INNER + inner
        count = gates.shape[1] // 3
        place = lax.broadcasted_iota(jnp.int32, (gates.shape[1], part), 0) % count
        chosen = jnp.where(place == expert, 1.0, 0.0).astype(bf16)
        weights = dot_tn(gates[slot], chosen)
        sigmoid = 1.0 / (1.0 + jnp.exp(-gate_act))
        silu = gate_act * sigmoid
        plain = silu * up_act
        act[slot, :, pl.ds(block * part, part)] = (weights * plain).astype(bf16)
        products = (plain * raw).astype(bf16)
        dots[slot, pl.ds(block, 1), :] = dot_nt(jnp.ones((8, part), bf16), products)[:1]
        hidden = weights * raw
        both[slot, :, pl.ds(block * 2 * part, part)] = (
            hidden * up_act * sigmoid * (1.0 + gate_act * (1.0 - sigmoid))
        ).astype(bf16)
        both[slot, :, pl.ds(block * 2 * part + part, part)] = (hidden * silu).astype(bf16)
        pair_grad = dot_tn(both[slot, :, pl.ds(block * 2 * part, 2 * part)], here)
        down_grad = dot_tn(act[slot, :, pl.ds(block * part, part)], grad_rows)

        @pl.when(order == 0)
        def _():
            total[: 2 * part] = pair_grad
            total[2 * part :] = down_grad

        @pl.when(order > 0)
        def _():
            total[: 2 * part] += pair_grad
            total[2 * part :] += down_grad

        @pl.when(step == 7)
        def _():
            stage_a[...] = total[...].astype(bf16)
            ring_copy(0).start()

        @pl.when(step == 15)
        def _():
            stage_b[...] = total[...].astype(bf16)

        @pl.when(step == 23)
        def _():
            ring_copy(0).wait()
            stage_b[...] = (stage_b[...].astype(f32) + ring[0].astype(f32)).astype(bf16)
            ring_copy(1).start()
            stage_a[...] = total[...].astype(bf16)
            local(stage_a, first_hbm, 0).start()

        @pl.when(step == 31)
        def _():
            local(stage_a, first_hbm, 0).wait()
            stage_a[...] = total[...].astype(bf16)

        return carry

    lax.fori_loop(0, 8 * outer_count, first_step, 0)
    for slot in range(1, 8):
        dots_copy(slot).start()
    for index in range(15):
        gather(index).wait_send()

    def second_step(order, carry):
        turn = order // 2
        there = jnp.where(turn == 0, 3, jnp.where(turn == 3, 0, turn))
        slot = there * 2 + 1 - order % 2
        dx_ref[...] = dot_nt(both[slot], wide[...])

        @pl.when(order % 2 == 0)
        def _():
            rows[slot] = dx_ref[...].astype(bf16)

        for index in range(4):

            @pl.when((order % 2 == 0) & (there == index))
            def _():
                back(index).start()

        @pl.when(order == 1)
        def _():
            back(3).wait_recv()
            rows[6] = (dx_ref[...] + core_in[3].astype(f32)).astype(bf16)
            back(4).start()
            back(5).start()

        @pl.when(order == 3)
        def _():
            back(1).wait_recv()
            back(5).wait_recv()
            rows[2, :half] = (dx_ref[:half] + core_in[1, :half].astype(f32)).astype(bf16)
            rows[2, half:] = (
                dx_ref[half:] + core_in[1, half:].astype(f32) + relay_in[1].astype(f32)
            ).astype(bf16)
            back(6).start()

        @pl.when(order == 5)
        def _():
            back(2).wait_recv()
            back(4).wait_recv()
            rows[4, :half] = (
                dx_ref[:half] + core_in[2, :half].astype(f32) + relay_in[0].astype(f32)
            ).astype(bf16)
            rows[4, half:] = (dx_ref[half:] + core_in[2, half:].astype(f32)).astype(bf16)
            back(7).start()

        return carry

    lax.fori_loop(0, 8, second_step, 0)

    def third_step(slot, carry):
        act[slot] = dot_nn(act[slot], down[...].reshape(outer_count * part, -1)).astype(bf16)
        pltpu.make_async_copy(act.at[slot], y_hbm.at[place_of(slot)], y_sem.at[slot]).start()
        return carry

    lax.fori_loop(0, 8, third_step, 0)
    ring_copy(1).wait()
    stage_a[...] = (stage_a[...].astype(f32) + ring[1].astype(f32)).astype(bf16)
    local(stage_a, last_hbm, 0).start()
    back(0).wait_recv()
    back(6).wait_recv()
    back(7).wait_recv()
    dx_ref[...] = (
        dx_ref[...]
        + core_in[0].astype(f32)
        + (last_in[0].astype(f32) + last_in[1].astype(f32))
    )
    local(dx_ref, dx_hbm, 1).start()
    dots_ref[0] = dots[0]
    for slot in range(1, 8):
        dots_copy(slot).wait()
        dots_ref[slot] = dots_in[slot]
    for index in range(8):
        back(index).wait_send()
    for index in range(4):
        weight(index).wait_send()
    for slot in range(8):
        pltpu.make_async_copy(act.at[slot], y_hbm.at[place_of(slot)], y_sem.at[slot]).wait()
    local(stage_a, last_hbm, 0).wait()
    local(dx_ref, dx_hbm, 1).wait()


def expert_layer(rows_own, gate_table, rows_grad, pair_own, down_own, outer_count):
    f32 = jnp.float32
    bf16 = jnp.bfloat16
    length, width = rows_own.shape
    part = down_own.shape[0]
    ahead = [(place, (place + 1) % outer_count) for place in range(outer_count)]
    pair_next = lax.ppermute(pair_own, "outer", ahead)
    down_next = lax.ppermute(down_own, "outer", ahead)
    anywhere = pl.BlockSpec(memory_space=pl.ANY)
    inside = pl.BlockSpec(memory_space=pltpu.VMEM)
    vmem, dma = pltpu.VMEM, pltpu.SemaphoreType.DMA
    hidden = outer_count * part
    share = jax.ShapeDtypeStruct((3 * part, width), bf16)
    dx, y_rows, dots, first, last = pl.pallas_call(
        functools.partial(expert_kernel, outer_count),
        out_shape=(
            jax.ShapeDtypeStruct((length, width), f32),
            jax.ShapeDtypeStruct((8, length, width), bf16),
            jax.ShapeDtypeStruct((8, 8, length), f32),
            share,
            share,
        ),
        in_specs=[anywhere] * 7,
        out_specs=(anywhere, anywhere, inside, anywhere, anywhere),
        scratch_shapes=[
            vmem((8, length, width), bf16),
            vmem((8,) + gate_table.shape, bf16),
            vmem((8, length, hidden), bf16),
            vmem((8, length, 2 * hidden), bf16),
            vmem((width, 2 * hidden), bf16),
            vmem((outer_count, part, width), bf16),
            vmem((2, length, width), bf16),
            vmem((3 * part, width), f32),
            vmem((3 * part, width), bf16),
            vmem((3 * part, width), bf16),
            vmem((2, 3 * part, width), bf16),
            vmem((4, length, width), bf16),
            vmem((2, length // 2, width), bf16),
            vmem((2, length, width), bf16),
            vmem((8, 8, length), f32),
            vmem((8, 8, length), f32),
            dma((6,)),
            dma((2,)),
            dma((8,)),
            dma((15,)),
            dma((15,)),
            dma((4,)),
            dma((4,)),
            dma((2,)),
            dma((2,)),
            dma((8,)),
            dma((8,)),
            dma((8,)),
            dma((8,)),
        ],
        compiler_params=pltpu.CompilerParams(
            collective_id=0, has_side_effects=True, vmem_limit_bytes=67043328
        ),
        cost_estimate=pl.CostEstimate(
            flops=18 * 8 * length * width * hidden, bytes_accessed=1 << 26, transcendentals=0
        ),
        name="expert_layer",
    )(rows_own, gate_table, rows_grad.reshape(8, length, width), pair_own, down_own, pair_next, down_next)
    last = lax.ppermute(last, "outer", ahead)
    return dx, y_rows.reshape(8 * length, width), dots, first, last


def on_device(
    hidden_in,
    segment_ids,
    expert_ids,
    attn_gain,
    w_query,
    w_key,
    w_value,
    w_out,
    ffn_gain,
    router,
    w_gate,
    w_up,
    w_down,
    grad_out,
):
    f32 = jnp.float32
    bf16 = jnp.bfloat16
    length, model_width = hidden_in.shape
    head_dim = HD
    head_count = w_query.shape[1] // head_dim
    kv_count = w_key.shape[1] // head_dim
    group_size = head_count // kv_count
    experts = router.shape[1]
    outer_count = experts // INNER
    here = ("inner", "narrow")
    fused = outer_count == 4 and lax.axis_size("narrow") == 2
    rows_grad = lax.all_gather(grad_out, here, axis=0, tiled=True)
    part = w_gate.shape[2]
    inputs = hidden_in.astype(f32)
    scale_one = norm_scale(inputs)
    normed = (inputs * scale_one * attn_gain).astype(bf16)
    query_pre = jnp.dot(normed, w_query, preferred_element_type=f32)
    key_pre = jnp.dot(normed, w_key, preferred_element_type=f32)
    value_pre = jnp.dot(normed, w_value, preferred_element_type=f32)
    cosine_table, sine_table = rope_tables(length, head_dim)
    query_rows = rotate(
        query_pre.reshape(length, head_count, head_dim), cosine_table, sine_table, 1.0
    ).astype(bf16)
    key_rows = rotate(
        key_pre.reshape(length, kv_count, head_dim), cosine_table, sine_table, 1.0
    ).astype(bf16)
    value_rows = value_pre.astype(bf16).reshape(length, kv_count, head_dim)
    grouped = query_rows.reshape(length, kv_count, group_size, head_dim)
    segments = segment_ids[0]
    places = jnp.arange(length, dtype=jnp.int32)
    allowed = (segments[:, None] == segments[None, :]) & (places[:, None] >= places[None, :])
    scores = attention_probs(grouped, key_rows, allowed, head_dim)
    row_max = jnp.max(scores, axis=-1, keepdims=True)
    log_total = row_max + jnp.log(jnp.sum(jnp.exp(scores - row_max), axis=-1, keepdims=True))
    weights_prob = jnp.exp(scores - log_total)
    attended = jnp.einsum(
        "ngqk,knd->qngd", weights_prob.astype(bf16), value_rows, preferred_element_type=f32
    )
    attended = attended.reshape(length, head_count * head_dim).astype(bf16)
    mixed_rows = inputs + jnp.dot(attended, w_out, preferred_element_type=f32)
    scale_two = norm_scale(mixed_rows)
    ffn_normed = (mixed_rows * scale_two * ffn_gain).astype(bf16)
    logits = jnp.dot(ffn_normed, router, preferred_element_type=f32)
    picked = expert_ids[:, :, None] == jnp.arange(experts, dtype=jnp.int32)[None, None, :]
    member = jnp.any(picked, axis=1)
    masked = jnp.where(member, logits, -jnp.inf)
    powers = jnp.where(member, jnp.exp(masked - jnp.max(masked, axis=-1, keepdims=True)), 0.0)
    gate_probs = powers / jnp.sum(powers, axis=-1, keepdims=True)
    if fused:
        table = gate_probs.T
        part_one = lax.reduce_precision(table, 8, 7)
        part_two = lax.reduce_precision(table - part_one, 8, 7)
        part_three = table - part_one - part_two
        table = jnp.concatenate([part_one, part_two, part_three], axis=0).astype(bf16)
        pair_own = jnp.concatenate([w_gate[0], w_up[0]], axis=1)
        rows_back, y_rows, dots, weight_first, weight_last = expert_layer(
            ffn_normed, table, rows_grad, pair_own, w_down[0], outer_count
        )
        moe_rows = lax.psum_scatter(y_rows, here, scatter_dimension=0, tiled=True)
        dots = dots[:, :outer_count].reshape(2, 2, 2, outer_count, length).sum(axis=1)
        each = jnp.arange(experts, dtype=jnp.int32)
        outer, inner = lax.axis_index("outer"), lax.axis_index("inner")
        side = (each % INNER // 2 + inner // 2) % 2
        core = (each + inner) % 2
        block = (outer + outer_count - each // INNER) % outer_count
        gate_grads = dots.reshape(experts, length)[(side * 2 + core) * outer_count + block].T
    else:
        full_gate = lax.all_gather(w_gate[0], "outer", axis=1, tiled=True)
        full_up = lax.all_gather(w_up[0], "outer", axis=1, tiled=True)
        full_down = lax.all_gather(w_down[0], "outer", axis=0, tiled=True)
        gate_table = lax.all_gather(gate_probs.T, here, axis=0, tiled=False)
        gate_table = gate_table.reshape(-1, outer_count, INNER, length)
        mine = lax.dynamic_index_in_dim(gate_table, lax.axis_index("inner"), 2, keepdims=False)
        row_gates = mine.transpose(0, 2, 1).reshape(-1, outer_count)
        gate_wide = jnp.repeat(row_gates, part, axis=1)
        rows_in = lax.all_gather(ffn_normed, here, axis=0, tiled=True)
        gate_act = jnp.dot(rows_in, full_gate, preferred_element_type=f32)
        up_act = jnp.dot(rows_in, full_up, preferred_element_type=f32)
        raw_grad = jnp.einsum("rd,fd->rf", rows_grad, full_down, preferred_element_type=f32)
        sigmoid_gate = jax.nn.sigmoid(gate_act)
        plain_act = gate_act * sigmoid_gate * up_act
        hidden_act = (gate_wide * plain_act).astype(bf16)
        hidden_grad = gate_wide * raw_grad
        moe_rows = lax.psum_scatter(
            jnp.dot(hidden_act, full_down, preferred_element_type=f32).astype(bf16),
            here,
            scatter_dimension=0,
            tiled=True,
        )
        gate_dots = jnp.sum((plain_act * raw_grad).reshape(-1, outer_count, part), axis=-1)
        lane = jnp.arange(INNER) == lax.axis_index("inner")
        gate_dots = jnp.where(lane[None, None, :], gate_dots[:, :, None], 0.0).reshape(-1, experts)
        gate_grads = lax.psum_scatter(gate_dots, here, scatter_dimension=0, tiled=True)
        gate_grad = (
            hidden_grad * up_act * sigmoid_gate * (1.0 + gate_act * (1.0 - sigmoid_gate))
        ).astype(bf16)
        up_grad = (hidden_grad * gate_act * sigmoid_gate).astype(bf16)
        copy_grads = (
            jnp.einsum("rf,df->rd", gate_grad, full_gate, preferred_element_type=f32)
            + jnp.einsum("rf,df->rd", up_grad, full_up, preferred_element_type=f32)
        ).astype(bf16)
        rows_back = lax.psum_scatter(copy_grads, here, scatter_dimension=0, tiled=True)
        down_w_grad = jnp.einsum("rf,rd->fd", hidden_act, rows_grad, preferred_element_type=f32)
        gate_w_grad = jnp.einsum("rd,rf->df", rows_in, gate_grad, preferred_element_type=f32)
        up_w_grad = jnp.einsum("rd,rf->df", rows_in, up_grad, preferred_element_type=f32)
        gate_w_grad, up_w_grad, down_w_grad = (
            lax.psum_scatter(gate_w_grad.astype(bf16), "outer", scatter_dimension=1, tiled=True),
            lax.psum_scatter(up_w_grad.astype(bf16), "outer", scatter_dimension=1, tiled=True),
            lax.psum_scatter(down_w_grad.astype(bf16), "outer", scatter_dimension=0, tiled=True),
        )
        gate_w_grad, up_w_grad, down_w_grad = (
            gate_w_grad[None].astype(f32),
            up_w_grad[None].astype(f32),
            down_w_grad[None].astype(f32),
        )
    cotangent = grad_out.astype(f32)
    logit_grads = (
        gate_probs * (gate_grads - jnp.sum(gate_probs * gate_grads, axis=-1, keepdims=True))
    ).astype(bf16)
    router_grad = jnp.einsum("sd,se->de", ffn_normed, logit_grads, preferred_element_type=f32)
    normed_two_grad = jnp.einsum("se,de->sd", logit_grads, router, preferred_element_type=f32)
    normed_two_grad = normed_two_grad + rows_back.astype(f32)
    mixed_part, ffn_gain_grad = norm_back(mixed_rows, scale_two, ffn_gain, normed_two_grad)
    mixed_grad = cotangent + mixed_part
    branch_grad = mixed_grad.astype(bf16)
    out_w_grad = jnp.einsum("sh,sd->hd", attended, branch_grad, preferred_element_type=f32)
    attended_grad = jnp.einsum("sd,hd->sh", branch_grad, w_out, preferred_element_type=f32).astype(
        bf16
    )
    attended_grad = attended_grad.reshape(length, kv_count, group_size, head_dim)
    scores = attention_probs(grouped, key_rows, allowed, head_dim)
    weights_prob = jnp.exp(scores - log_total)
    value_grad = jnp.einsum(
        "ngqk,qngd->knd", weights_prob.astype(bf16), attended_grad, preferred_element_type=f32
    )
    prob_grad = jnp.einsum("qngd,knd->ngqk", attended_grad, value_rows, preferred_element_type=f32)
    score_grad = (
        weights_prob * (prob_grad - jnp.sum(weights_prob * prob_grad, axis=-1, keepdims=True))
    ).astype(bf16)
    query_grad = jnp.einsum(
        "ngqk,knd->qngd", score_grad, key_rows, preferred_element_type=f32
    ) * head_dim ** (-0.5)
    key_grad = jnp.einsum(
        "ngqk,qngd->knd", score_grad, grouped, preferred_element_type=f32
    ) * head_dim ** (-0.5)
    query_grad = rotate(
        query_grad.reshape(length, head_count, head_dim), cosine_table, sine_table, -1.0
    )
    query_grad = query_grad.reshape(length, -1).astype(bf16)
    key_grad = rotate(key_grad, cosine_table, sine_table, -1.0).reshape(length, -1).astype(bf16)
    value_grad = value_grad.reshape(length, -1).astype(bf16)
    query_w_grad = jnp.einsum("sd,sh->dh", normed, query_grad, preferred_element_type=f32)
    key_w_grad = jnp.einsum("sd,sh->dh", normed, key_grad, preferred_element_type=f32)
    value_w_grad = jnp.einsum("sd,sh->dh", normed, value_grad, preferred_element_type=f32)
    normed_one_grad = (
        jnp.einsum("sh,dh->sd", query_grad, w_query, preferred_element_type=f32)
        + jnp.einsum("sh,dh->sd", key_grad, w_key, preferred_element_type=f32)
        + jnp.einsum("sh,dh->sd", value_grad, w_value, preferred_element_type=f32)
    )
    input_part, attn_gain_grad = norm_back(inputs, scale_one, attn_gain, normed_one_grad)
    grad_in = (mixed_grad + input_part).astype(bf16)
    everywhere = ("outer", "inner", "narrow")
    small = jnp.concatenate(
        [router_grad, attn_gain_grad[:, None], ffn_gain_grad[:, None]], axis=1
    )
    small = jnp.pad(small, ((0, 0), (0, 128 - small.shape[1])))
    columns = jnp.concatenate(
        [query_w_grad, key_w_grad, value_w_grad, out_w_grad, small], axis=1
    ).astype(bf16)
    mixed_late, columns = lax.optimization_barrier((mixed_rows, columns))
    hidden_out = (mixed_late + moe_rows.astype(f32)).astype(bf16)
    if fused:
        columns, hidden_out, weight_last = lax.optimization_barrier(
            (columns, hidden_out, weight_last)
        )
        weight_sum = weight_first.astype(f32) + weight_last.astype(f32)
        gate_w_grad = weight_sum[:part].T[None]
        up_w_grad = weight_sum[part : 2 * part].T[None]
        down_w_grad = weight_sum[2 * part :][None]
    shares = lax.psum_scatter(columns, everywhere, scatter_dimension=0, tiled=True)
    columns = lax.all_gather(shares, everywhere, axis=0, tiled=True).astype(f32)
    starts = [0]
    for width in (w_query.shape[1], w_key.shape[1], w_value.shape[1], model_width, experts, 1, 1):
        starts.append(starts[-1] + width)
    pieces = [columns[:, low:high] for low, high in zip(starts[:-1], starts[1:])]
    summed = (
        pieces[5][:, 0],
        pieces[0],
        pieces[1],
        pieces[2],
        pieces[3],
        pieces[6][:, 0],
        pieces[4],
    )
    return (
        hidden_out,
        grad_in,
        summed[0],
        summed[1],
        summed[2],
        summed[3],
        summed[4],
        summed[5],
        summed[6],
        gate_w_grad,
        up_w_grad,
        down_w_grad,
    )


def solution(mesh):
    names = ("outer", "inner", "narrow")
    narrow = mesh.shape["narrow"]
    cut = Mesh(mesh.devices.reshape(-1, INNER, narrow), names)
    rows = P(names, None)
    columns = P(("outer", "inner"), None, "narrow")
    depths = P(("outer", "inner"), "narrow", None)
    return jax.shard_map(
        on_device,
        mesh=cut,
        in_specs=(rows, rows, rows) + (P(),) * 7 + (columns, columns, depths, rows),
        out_specs=(rows, rows) + (P(),) * 7 + (columns, columns, depths),
        check_vma=False,
    )
```

```python
import functools

import jax
import jax.numpy as jnp
from jax import lax
from jax.experimental import pallas as pl
from jax.experimental.pallas import tpu as pltpu
from jax.sharding import Mesh
from jax.sharding import PartitionSpec as P

HD = 64
INNER = 4


EPSILON = 1e-05


def norm_scale(values):
    return lax.rsqrt(jnp.mean(values * values, axis=-1, keepdims=True) + EPSILON)


def norm_back(values, inv_rms, gain_vector, grad_rows):
    weighted = grad_rows * gain_vector
    inner = jnp.mean(weighted * values, axis=-1, keepdims=True)
    value_grad = inv_rms * weighted - values * (inv_rms * inv_rms * inv_rms) * inner
    return (value_grad, jnp.sum(grad_rows * values * inv_rms, axis=0))


def rope_tables(length, head_dim):
    half_size = head_dim // 2
    freqs = 10000.0 ** (-(jnp.arange(half_size, dtype=jnp.float32) * 2.0) / head_dim)
    angles = jnp.arange(length, dtype=jnp.float32)[:, None] * freqs[None, :]
    return (jnp.cos(angles), jnp.sin(angles))


def rotate(values, cosine_table, sine_table, direction):
    half_size = values.shape[-1] // 2
    first_half = values[..., :half_size]
    second_half = values[..., half_size:]
    cosine_part = cosine_table[:, None, :]
    sine_part = sine_table[:, None, :] * direction
    return jnp.concatenate(
        [
            first_half * cosine_part - second_half * sine_part,
            second_half * cosine_part + first_half * sine_part,
        ],
        axis=-1,
    )


def attention_probs(grouped, key_rows, allowed, head_dim):
    scores = jnp.einsum(
        "qngd,knd->ngqk", grouped, key_rows, preferred_element_type=jnp.float32
    ) * head_dim ** (-0.5)
    return jnp.where(allowed, scores, -1e30)


def dot_nn(left, right):
    return lax.dot_general(left, right, (((1,), (0,)), ((), ())), preferred_element_type=jnp.float32)


def dot_nt(left, right):
    return lax.dot_general(left, right, (((1,), (1,)), ((), ())), preferred_element_type=jnp.float32)


def dot_tn(left, right):
    return lax.dot_general(left, right, (((0,), (0,)), ((), ())), preferred_element_type=jnp.float32)


def expert_kernel(
    outer_count,
    x_hbm,
    gate_hbm,
    grad_hbm,
    pair_own,
    down_own,
    pair_next,
    down_next,
    dx_hbm,
    y_hbm,
    dots_ref,
    first_hbm,
    last_hbm,
    rows,
    gates,
    act,
    both,
    wide,
    down,
    grads,
    total,
    stage_a,
    stage_b,
    ring,
    core_in,
    relay_in,
    last_in,
    dots,
    dots_in,
    local_sem,
    grad_sem,
    y_sem,
    gather_send,
    gather_recv,
    weight_send,
    weight_recv,
    ring_send,
    ring_recv,
    dots_send,
    dots_recv,
    back_send,
    back_recv,
):
    f32 = jnp.float32
    bf16 = jnp.bfloat16
    length, part = rows.shape[1], down.shape[1]
    half = length // 2
    outer, inner, narrow = lax.axis_index("outer"), lax.axis_index("inner"), lax.axis_index("narrow")
    side, core = inner // 2, inner % 2
    core_at = {"inner": side * 2 + (1 - core)}
    x_at = {"narrow": 1 - narrow}
    y_at = {"inner": (1 - side) * 2 + core}
    next_at = {"outer": lax.rem(outer + 1, outer_count)}
    before_at = {"outer": lax.rem(outer + outer_count - 1, outer_count)}

    def device_of(slot):
        there = slot // 2
        return {
            "inner": ((side + there // 2) % 2) * 2 + (core + slot % 2) % 2,
            "narrow": (narrow + there % 2) % 2,
        }

    def place_of(slot):
        there = slot // 2
        at_inner = ((side + there // 2) % 2) * 2 + (core + slot % 2) % 2
        return at_inner * 2 + (narrow + there % 2) % 2

    def remote(source, target, sends, recvs, index, device):
        return pltpu.make_async_remote_copy(
            src_ref=source,
            dst_ref=target,
            send_sem=sends.at[index],
            recv_sem=recvs.at[index],
            device_id=device,
            device_id_type=pl.DeviceIdType.MESH,
        )

    def local(source, target, index):
        return pltpu.make_async_copy(source, target, local_sem.at[index])

    low, high = pl.ds(0, half), pl.ds(half, half)
    dx_ref = total.at[pl.ds(0, length)]

    def gather(index):
        source, target, device = (
            (rows.at[0], rows.at[1], core_at),
            (rows.at[0], rows.at[2], x_at),
            (rows.at[0], rows.at[4], y_at),
            (rows.at[2, low], rows.at[6, low], y_at),
            (rows.at[4, high], rows.at[6, high], x_at),
            (rows.at[2], rows.at[3], core_at),
            (rows.at[4], rows.at[5], core_at),
            (rows.at[6], rows.at[7], core_at),
            (gates.at[0], gates.at[1], core_at),
            (gates.at[0], gates.at[2], x_at),
            (gates.at[0], gates.at[4], y_at),
            (gates.at[0], gates.at[6], device_of(6)),
            (gates.at[2], gates.at[3], core_at),
            (gates.at[4], gates.at[5], core_at),
            (gates.at[6], gates.at[7], core_at),
        )[index]
        return remote(source, target, gather_send, gather_recv, index, device)

    def wide_at(slot):
        return wide.at[:, pl.ds(slot * 2 * part, 2 * part)]

    def weight(index):
        slot = 1 + index // 2
        if index % 2 == 0:
            return remote(
                wide_at(slot), wide_at(slot + 1), weight_send, weight_recv, index, next_at
            )
        return remote(
            down.at[slot], down.at[slot + 1], weight_send, weight_recv, index, next_at
        )

    def ring_copy(index):
        source = (stage_a, stage_b)[index]
        return remote(source, ring.at[index], ring_send, ring_recv, index, next_at)

    def dots_copy(slot):
        return remote(
            dots.at[slot], dots_in.at[slot], dots_send, dots_recv, slot, device_of(slot)
        )

    def back(index):
        source, target, device = (
            (rows.at[1], core_in.at[0], core_at),
            (rows.at[3], core_in.at[1], core_at),
            (rows.at[5], core_in.at[2], core_at),
            (rows.at[7], core_in.at[3], core_at),
            (rows.at[6, low], relay_in.at[0], x_at),
            (rows.at[6, high], relay_in.at[1], y_at),
            (rows.at[2], last_in.at[0], x_at),
            (rows.at[4], last_in.at[1], y_at),
        )[index]
        return remote(source, target, back_send, back_recv, index, device)

    own_copies = (
        local(x_hbm, rows.at[0], 0),
        local(gate_hbm, gates.at[0], 1),
        local(pair_next, wide_at(1), 2),
        local(down_next, down.at[1], 3),
        local(pair_own, wide_at(0), 4),
        local(down_own, down.at[0], 5),
    )
    for copy in own_copies:
        copy.start()

    def fetch(step):
        order = step % 8
        slot = jnp.where(order == 3, 4, jnp.where(order == 4, 3, order))
        return pltpu.make_async_copy(
            grad_hbm.at[place_of(slot)], grads.at[step % 2], grad_sem.at[step % 2]
        )

    fetch(0).start()
    barrier = pltpu.get_barrier_semaphore()
    for slot in range(1, 8):
        pl.semaphore_signal(
            barrier, inc=1, device_id=device_of(slot), device_id_type=pl.DeviceIdType.MESH
        )
    for device in (next_at, before_at):
        pl.semaphore_signal(
            barrier, inc=1, device_id=device, device_id_type=pl.DeviceIdType.MESH
        )
    pl.semaphore_wait(barrier, 9)
    own_copies[0].wait()
    own_copies[1].wait()
    for index in (1, 2, 9, 10, 11, 0, 8):
        gather(index).start()
    for copy in own_copies[2:]:
        copy.wait()
    weight(0).start()
    weight(1).start()

    def first_step(step, carry):
        turn, order = step // 8, step % 8
        slot = jnp.where(order == 3, 4, jnp.where(order == 4, 3, order))
        block = jnp.where(turn == 0, 1, jnp.where(turn == 1, 2, jnp.where(turn == 2, 0, 3)))

        @pl.when(step + 1 < 8 * outer_count)
        def _():
            fetch(step + 1).start()

        @pl.when(step == 1)
        def _():
            gather(0).wait_recv()
            gather(8).wait_recv()

        @pl.when(step == 2)
        def _():
            gather(1).wait_recv()
            gather(3).start()
            gather(5).start()
            gather(2).wait_recv()
            gather(4).start()
            gather(6).start()
            gather(9).wait_recv()
            gather(12).start()
            gather(10).wait_recv()
            gather(13).start()

        @pl.when(step == 4)
        def _():
            gather(5).wait_recv()
            gather(12).wait_recv()

        @pl.when(step == 5)
        def _():
            gather(6).wait_recv()
            gather(13).wait_recv()

        @pl.when(step == 6)
        def _():
            gather(3).wait_recv()
            gather(4).wait_recv()
            gather(7).start()
            gather(11).wait_recv()
            gather(14).start()

        @pl.when(step == 7)
        def _():
            gather(7).wait_recv()
            gather(14).wait_recv()

        @pl.when(step == 8)
        def _():
            weight(0).wait_recv()
            weight(1).wait_recv()
            weight(2).start()
            weight(3).start()

        @pl.when(step == 24)
        def _():
            weight(2).wait_recv()
            weight(3).wait_recv()

        fetch(step).wait()
        here = rows[slot]
        grad_rows = grads[step % 2]
        products = dot_nn(here, wide[:, pl.ds(block * 2 * part, 2 * part)])
        gate_act, up_act = products[:, :part], products[:, part:]
        raw = dot_nt(grad_rows, down[block])
        expert = lax.rem(outer + outer_count - block, outer_count) * INNER + inner
        count = gates.shape[1] // 3
        place = lax.broadcasted_iota(jnp.int32, (gates.shape[1], part), 0) % count
        chosen = jnp.where(place == expert, 1.0, 0.0).astype(bf16)
        weights = dot_tn(gates[slot], chosen)
        sigmoid = 1.0 / (1.0 + jnp.exp(-gate_act))
        silu = gate_act * sigmoid
        plain = silu * up_act
        act[slot, :, pl.ds(block * part, part)] = (weights * plain).astype(bf16)
        products = (plain * raw).astype(bf16)
        dots[slot, pl.ds(block, 1), :] = dot_nt(jnp.ones((8, part), bf16), products)[:1]
        hidden = weights * raw
        both[slot, :, pl.ds(block * 2 * part, part)] = (
            hidden * up_act * sigmoid * (1.0 + gate_act * (1.0 - sigmoid))
        ).astype(bf16)
        both[slot, :, pl.ds(block * 2 * part + part, part)] = (hidden * silu).astype(bf16)
        pair_grad = dot_tn(both[slot, :, pl.ds(block * 2 * part, 2 * part)], here)
        down_grad = dot_tn(act[slot, :, pl.ds(block * part, part)], grad_rows)

        @pl.when(order == 0)
        def _():
            total[: 2 * part] = pair_grad
            total[2 * part :] = down_grad

        @pl.when(order > 0)
        def _():
            total[: 2 * part] += pair_grad
            total[2 * part :] += down_grad

        @pl.when(step == 7)
        def _():
            stage_a[...] = total[...].astype(bf16)
            ring_copy(0).start()

        @pl.when(step == 15)
        def _():
            stage_b[...] = total[...].astype(bf16)

        @pl.when(step == 23)
        def _():
            ring_copy(0).wait()
            stage_b[...] = (stage_b[...].astype(f32) + ring[0].astype(f32)).astype(bf16)
            ring_copy(1).start()
            stage_a[...] = total[...].astype(bf16)
            local(stage_a, first_hbm, 0).start()

        @pl.when(step == 31)
        def _():
            local(stage_a, first_hbm, 0).wait()
            stage_a[...] = total[...].astype(bf16)

        return carry

    lax.fori_loop(0, 8 * outer_count, first_step, 0)
    for slot in range(1, 8):
        dots_copy(slot).start()
    for index in range(15):
        gather(index).wait_send()

    def second_step(order, carry):
        turn = order // 2
        there = jnp.where(turn == 0, 3, jnp.where(turn == 3, 0, turn))
        slot = there * 2 + 1 - order % 2
        dx_ref[...] = dot_nt(both[slot], wide[...])

        @pl.when(order % 2 == 0)
        def _():
            rows[slot] = dx_ref[...].astype(bf16)

        for index in range(4):

            @pl.when((order % 2 == 0) & (there == index))
            def _():
                back(index).start()

        @pl.when(order == 1)
        def _():
            back(3).wait_recv()
            rows[6] = (dx_ref[...] + core_in[3].astype(f32)).astype(bf16)
            back(4).start()
            back(5).start()

        @pl.when(order == 3)
        def _():
            back(1).wait_recv()
            back(5).wait_recv()
            rows[2, :half] = (dx_ref[:half] + core_in[1, :half].astype(f32)).astype(bf16)
            rows[2, half:] = (
                dx_ref[half:] + core_in[1, half:].astype(f32) + relay_in[1].astype(f32)
            ).astype(bf16)
            back(6).start()

        @pl.when(order == 5)
        def _():
            back(2).wait_recv()
            back(4).wait_recv()
            rows[4, :half] = (
                dx_ref[:half] + core_in[2, :half].astype(f32) + relay_in[0].astype(f32)
            ).astype(bf16)
            rows[4, half:] = (dx_ref[half:] + core_in[2, half:].astype(f32)).astype(bf16)
            back(7).start()

        return carry

    lax.fori_loop(0, 8, second_step, 0)

    def third_step(slot, carry):
        act[slot] = dot_nn(act[slot], down[...].reshape(outer_count * part, -1)).astype(bf16)
        pltpu.make_async_copy(act.at[slot], y_hbm.at[place_of(slot)], y_sem.at[slot]).start()
        return carry

    lax.fori_loop(0, 8, third_step, 0)
    ring_copy(1).wait()
    stage_a[...] = (stage_a[...].astype(f32) + ring[1].astype(f32)).astype(bf16)
    local(stage_a, last_hbm, 0).start()
    back(0).wait_recv()
    back(6).wait_recv()
    back(7).wait_recv()
    dx_ref[...] = (
        dx_ref[...]
        + core_in[0].astype(f32)
        + (last_in[0].astype(f32) + last_in[1].astype(f32))
    )
    local(dx_ref, dx_hbm, 1).start()
    dots_ref[0] = dots[0]
    for slot in range(1, 8):
        dots_copy(slot).wait()
        dots_ref[slot] = dots_in[slot]
    for index in range(8):
        back(index).wait_send()
    for index in range(4):
        weight(index).wait_send()
    for slot in range(8):
        pltpu.make_async_copy(act.at[slot], y_hbm.at[place_of(slot)], y_sem.at[slot]).wait()
    local(stage_a, last_hbm, 0).wait()
    local(dx_ref, dx_hbm, 1).wait()


def expert_layer(rows_own, gate_table, rows_grad, pair_own, down_own, outer_count):
    f32 = jnp.float32
    bf16 = jnp.bfloat16
    length, width = rows_own.shape
    part = down_own.shape[0]
    ahead = [(place, (place + 1) % outer_count) for place in range(outer_count)]
    pair_next = lax.ppermute(pair_own, "outer", ahead)
    down_next = lax.ppermute(down_own, "outer", ahead)
    anywhere = pl.BlockSpec(memory_space=pl.ANY)
    inside = pl.BlockSpec(memory_space=pltpu.VMEM)
    vmem, dma = pltpu.VMEM, pltpu.SemaphoreType.DMA
    hidden = outer_count * part
    share = jax.ShapeDtypeStruct((3 * part, width), bf16)
    dx, y_rows, dots, first, last = pl.pallas_call(
        functools.partial(expert_kernel, outer_count),
        out_shape=(
            jax.ShapeDtypeStruct((length, width), f32),
            jax.ShapeDtypeStruct((8, length, width), bf16),
            jax.ShapeDtypeStruct((8, 8, length), f32),
            share,
            share,
        ),
        in_specs=[anywhere] * 7,
        out_specs=(anywhere, anywhere, inside, anywhere, anywhere),
        scratch_shapes=[
            vmem((8, length, width), bf16),
            vmem((8,) + gate_table.shape, bf16),
            vmem((8, length, hidden), bf16),
            vmem((8, length, 2 * hidden), bf16),
            vmem((width, 2 * hidden), bf16),
            vmem((outer_count, part, width), bf16),
            vmem((2, length, width), bf16),
            vmem((3 * part, width), f32),
            vmem((3 * part, width), bf16),
            vmem((3 * part, width), bf16),
            vmem((2, 3 * part, width), bf16),
            vmem((4, length, width), bf16),
            vmem((2, length // 2, width), bf16),
            vmem((2, length, width), bf16),
            vmem((8, 8, length), f32),
            vmem((8, 8, length), f32),
            dma((6,)),
            dma((2,)),
            dma((8,)),
            dma((15,)),
            dma((15,)),
            dma((4,)),
            dma((4,)),
            dma((2,)),
            dma((2,)),
            dma((8,)),
            dma((8,)),
            dma((8,)),
            dma((8,)),
        ],
        compiler_params=pltpu.CompilerParams(
            collective_id=0, has_side_effects=True, vmem_limit_bytes=67043328
        ),
        cost_estimate=pl.CostEstimate(
            flops=18 * 8 * length * width * hidden, bytes_accessed=1 << 26, transcendentals=0
        ),
        name="expert_layer",
    )(rows_own, gate_table, rows_grad.reshape(8, length, width), pair_own, down_own, pair_next, down_next)
    last = lax.ppermute(last, "outer", ahead)
    return dx, y_rows.reshape(8 * length, width), dots, first, last


def reduce_kernel(
    outer_count,
    normed_ref,
    turned_ref,
    attended_ref,
    branch_ref,
    small_ref,
    out_one,
    out_two,
    out_three,
    out_four,
    work_one,
    work_two,
    work_three,
    work_four,
    core_one,
    core_two,
    core_three,
    core_four,
    near_one,
    near_two,
    near_three,
    near_four,
    far_one,
    far_two,
    far_three,
    far_four,
    deep_one,
    deep_two,
    deep_three,
    deep_four,
    sends,
    recvs,
    deep_sends,
    deep_recvs,
):
    f32 = jnp.float32
    bf16 = jnp.bfloat16
    outer, inner, narrow = lax.axis_index("outer"), lax.axis_index("inner"), lax.axis_index("narrow")
    side, core = inner // 2, inner % 2
    core_at = {"inner": side * 2 + (1 - core)}
    x_at = {"narrow": 1 - narrow}
    y_at = {"inner": (1 - side) * 2 + core}
    outs = (out_one, out_two, out_three, out_four)
    works = (work_one, work_two, work_three, work_four)
    cores = (core_one, core_two, core_three, core_four)
    nears = (near_one, near_two, near_three, near_four)
    fars = (far_one, far_two, far_three, far_four)
    deeps = (deep_one, deep_two, deep_three, deep_four)
    rows = work_one.shape[0]
    halves, quarters, eighths = rows // 2, rows // 4, rows // 8
    pieces = eighths // outer_count

    def span(start, size):
        return pl.ds(pl.multiple_of(start, pieces), size)

    def remote(source, target, chunk, stage, device):
        return pltpu.make_async_remote_copy(
            src_ref=source,
            dst_ref=target,
            send_sem=sends.at[chunk * 8 + stage],
            recv_sem=recvs.at[chunk * 8 + stage],
            device_id=device,
            device_id_type=pl.DeviceIdType.MESH,
        )

    def places(chunk):
        first, second = (narrow, side) if chunk % 2 == 0 else (side, narrow)
        devices = (x_at, y_at) if chunk % 2 == 0 else (y_at, x_at)
        at_core = core * halves
        at_near = at_core + first * quarters
        at_far = at_near + second * eighths
        return first, second, devices, at_core, at_near, at_far

    def copies(chunk, stage):
        first, second, devices, at_core, at_near, at_far = places(chunk)
        work, out = works[chunk], outs[chunk]
        if stage == 0:
            source = work.at[span((1 - core) * halves, halves)]
            return [remote(source, cores[chunk], chunk, 0, core_at)]
        if stage == 1:
            source = work.at[span(at_core + (1 - first) * quarters, quarters)]
            return [remote(source, nears[chunk], chunk, 1, devices[0])]
        if stage == 2:
            source = work.at[span(at_near + (1 - second) * eighths, eighths)]
            return [remote(source, fars[chunk], chunk, 2, devices[1])]
        if stage in (3, 4):
            found = []
            for step in range(1, outer_count):
                there = lax.rem(outer + step, outer_count)
                index = (chunk * 2 + stage - 3) * (outer_count - 1) + step - 1
                if stage == 3:
                    source = work.at[span(at_far + there * pieces, pieces)]
                    target = deeps[chunk].at[step - 1]
                else:
                    source = out.at[span(at_far + outer * pieces, pieces)]
                    target = source
                found.append(
                    pltpu.make_async_remote_copy(
                        src_ref=source,
                        dst_ref=target,
                        send_sem=deep_sends.at[index],
                        recv_sem=deep_recvs.at[index],
                        device_id={"outer": there},
                        device_id_type=pl.DeviceIdType.MESH,
                    )
                )
            return found
        start, size, device = (
            (at_far, eighths, devices[1]),
            (at_near, quarters, devices[0]),
            (at_core, halves, core_at),
        )[stage - 5]
        source = out.at[span(start, size)]
        return [remote(source, source, chunk, stage, device)]

    def arrive(chunk, stage):
        first, second, devices, at_core, at_near, at_far = places(chunk)
        work, out = works[chunk], outs[chunk]
        for copy in copies(chunk, stage):
            copy.wait_recv()
        if stage < 3:
            start, size, box = (
                (at_core, halves, cores[chunk]),
                (at_near, quarters, nears[chunk]),
                (at_far, eighths, fars[chunk]),
            )[stage]
            held = work[span(start, size)].astype(f32) + box[...].astype(f32)
            work[span(start, size)] = held.astype(bf16)
        elif stage == 3:
            held = work[span(at_far + outer * pieces, pieces)].astype(f32)
            for step in range(outer_count - 1):
                held = held + deeps[chunk][step].astype(f32)
            out[span(at_far + outer * pieces, pieces)] = held.astype(bf16)

    barrier = pltpu.get_barrier_semaphore()
    others = [core_at, x_at, y_at]
    for step in range(1, outer_count):
        others.append({"outer": lax.rem(outer + step, outer_count)})
    for device in others:
        pl.semaphore_signal(
            barrier, inc=1, device_id=device, device_id_type=pl.DeviceIdType.MESH
        )
    width = small_ref.shape[1]
    model = normed_ref.shape[1]
    heads = attended_ref.shape[1]
    kept = (turned_ref.shape[1] - heads) // 2

    def product(chunk):
        if chunk == 0:
            work_one[...] = dot_tn(attended_ref[...], branch_ref[...]).astype(bf16)
        elif chunk == 1:
            work_two[...] = dot_tn(normed_ref[...], turned_ref[:, :heads]).astype(bf16)
        elif chunk == 2:
            work_three[...] = dot_tn(
                normed_ref[...], turned_ref[:, heads : heads + kept]
            ).astype(bf16)
        else:
            work_four[:, :kept] = dot_tn(
                normed_ref[...], turned_ref[:, heads + kept :]
            ).astype(bf16)
            work_four[:, kept:] = small_ref[...].astype(bf16)

    product(0)
    pl.semaphore_wait(barrier, 2 + outer_count)
    for slot in range(8 + 4):
        for chunk in range(4):
            stage = slot - chunk
            if stage > 0 and stage <= 8:
                arrive(chunk, stage - 1)
            if stage == 0 and chunk > 0:
                product(chunk)
            if 0 <= stage < 8:
                for copy in copies(chunk, stage):
                    copy.start()
    for chunk in range(4):
        for stage in range(8):
            for copy in copies(chunk, stage):
                copy.wait_send()


def reduce_layer(normed, turned, attended, branch, small, outer_count):
    bf16 = jnp.bfloat16
    model, heads = normed.shape[1], attended.shape[1]
    kept = (turned.shape[1] - heads) // 2
    tops = [heads, model, model, model]
    widths = [model, heads, kept, kept + small.shape[1]]
    vmem, dma = pltpu.VMEM, pltpu.SemaphoreType.DMA
    inside = pl.BlockSpec(memory_space=pltpu.VMEM)
    scratch = []
    for cut in (1, 2, 4, 8):
        scratch += [vmem((top // cut, width), bf16) for top, width in zip(tops, widths)]
    scratch += [
        vmem((outer_count - 1, top // 8 // outer_count, width), bf16)
        for top, width in zip(tops, widths)
    ]
    return pl.pallas_call(
        functools.partial(reduce_kernel, outer_count),
        out_shape=tuple(
            jax.ShapeDtypeStruct((top, width), bf16) for top, width in zip(tops, widths)
        ),
        in_specs=[inside] * 5,
        out_specs=(inside,) * 4,
        scratch_shapes=scratch
        + [dma((32,)), dma((32,)), dma((8 * (outer_count - 1),)), dma((8 * (outer_count - 1),))],
        compiler_params=pltpu.CompilerParams(
            collective_id=1, has_side_effects=True, vmem_limit_bytes=60 << 20
        ),
        name="reduce_layer",
    )(normed, turned, attended, branch, small)


def on_device(
    hidden_in,
    segment_ids,
    expert_ids,
    attn_gain,
    w_query,
    w_key,
    w_value,
    w_out,
    ffn_gain,
    router,
    w_gate,
    w_up,
    w_down,
    grad_out,
):
    f32 = jnp.float32
    bf16 = jnp.bfloat16
    length, model_width = hidden_in.shape
    head_dim = HD
    head_count = w_query.shape[1] // head_dim
    kv_count = w_key.shape[1] // head_dim
    group_size = head_count // kv_count
    experts = router.shape[1]
    outer_count = experts // INNER
    here = ("inner", "narrow")
    fused = outer_count == 4 and lax.axis_size("narrow") == 2
    rows_grad = lax.all_gather(grad_out, here, axis=0, tiled=True)
    part = w_gate.shape[2]
    inputs = hidden_in.astype(f32)
    scale_one = norm_scale(inputs)
    normed = (inputs * scale_one * attn_gain).astype(bf16)
    query_pre = jnp.dot(normed, w_query, preferred_element_type=f32)
    key_pre = jnp.dot(normed, w_key, preferred_element_type=f32)
    value_pre = jnp.dot(normed, w_value, preferred_element_type=f32)
    cosine_table, sine_table = rope_tables(length, head_dim)
    query_rows = rotate(
        query_pre.reshape(length, head_count, head_dim), cosine_table, sine_table, 1.0
    ).astype(bf16)
    key_rows = rotate(
        key_pre.reshape(length, kv_count, head_dim), cosine_table, sine_table, 1.0
    ).astype(bf16)
    value_rows = value_pre.astype(bf16).reshape(length, kv_count, head_dim)
    grouped = query_rows.reshape(length, kv_count, group_size, head_dim)
    segments = segment_ids[0]
    places = jnp.arange(length, dtype=jnp.int32)
    allowed = (segments[:, None] == segments[None, :]) & (places[:, None] >= places[None, :])
    scores = attention_probs(grouped, key_rows, allowed, head_dim)
    row_max = jnp.max(scores, axis=-1, keepdims=True)
    log_total = row_max + jnp.log(jnp.sum(jnp.exp(scores - row_max), axis=-1, keepdims=True))
    weights_prob = jnp.exp(scores - log_total)
    attended = jnp.einsum(
        "ngqk,knd->qngd", weights_prob.astype(bf16), value_rows, preferred_element_type=f32
    )
    attended = attended.reshape(length, head_count * head_dim).astype(bf16)
    mixed_rows = inputs + jnp.dot(attended, w_out, preferred_element_type=f32)
    scale_two = norm_scale(mixed_rows)
    ffn_normed = (mixed_rows * scale_two * ffn_gain).astype(bf16)
    logits = jnp.dot(ffn_normed, router, preferred_element_type=f32)
    picked = expert_ids[:, :, None] == jnp.arange(experts, dtype=jnp.int32)[None, None, :]
    member = jnp.any(picked, axis=1)
    masked = jnp.where(member, logits, -jnp.inf)
    powers = jnp.where(member, jnp.exp(masked - jnp.max(masked, axis=-1, keepdims=True)), 0.0)
    gate_probs = powers / jnp.sum(powers, axis=-1, keepdims=True)
    if fused:
        table = gate_probs.T
        part_one = lax.reduce_precision(table, 8, 7)
        part_two = lax.reduce_precision(table - part_one, 8, 7)
        part_three = table - part_one - part_two
        table = jnp.concatenate([part_one, part_two, part_three], axis=0).astype(bf16)
        pair_own = jnp.concatenate([w_gate[0], w_up[0]], axis=1)
        rows_back, y_rows, dots, weight_first, weight_last = expert_layer(
            ffn_normed, table, rows_grad, pair_own, w_down[0], outer_count
        )
        moe_rows = lax.psum_scatter(y_rows, here, scatter_dimension=0, tiled=True)
        dots = dots[:, :outer_count].reshape(2, 2, 2, outer_count, length).sum(axis=1)
        each = jnp.arange(experts, dtype=jnp.int32)
        outer, inner = lax.axis_index("outer"), lax.axis_index("inner")
        side = (each % INNER // 2 + inner // 2) % 2
        core = (each + inner) % 2
        block = (outer + outer_count - each // INNER) % outer_count
        gate_grads = dots.reshape(experts, length)[(side * 2 + core) * outer_count + block].T
    else:
        full_gate = lax.all_gather(w_gate[0], "outer", axis=1, tiled=True)
        full_up = lax.all_gather(w_up[0], "outer", axis=1, tiled=True)
        full_down = lax.all_gather(w_down[0], "outer", axis=0, tiled=True)
        gate_table = lax.all_gather(gate_probs.T, here, axis=0, tiled=False)
        gate_table = gate_table.reshape(-1, outer_count, INNER, length)
        mine = lax.dynamic_index_in_dim(gate_table, lax.axis_index("inner"), 2, keepdims=False)
        row_gates = mine.transpose(0, 2, 1).reshape(-1, outer_count)
        gate_wide = jnp.repeat(row_gates, part, axis=1)
        rows_in = lax.all_gather(ffn_normed, here, axis=0, tiled=True)
        gate_act = jnp.dot(rows_in, full_gate, preferred_element_type=f32)
        up_act = jnp.dot(rows_in, full_up, preferred_element_type=f32)
        raw_grad = jnp.einsum("rd,fd->rf", rows_grad, full_down, preferred_element_type=f32)
        sigmoid_gate = jax.nn.sigmoid(gate_act)
        plain_act = gate_act * sigmoid_gate * up_act
        hidden_act = (gate_wide * plain_act).astype(bf16)
        hidden_grad = gate_wide * raw_grad
        moe_rows = lax.psum_scatter(
            jnp.dot(hidden_act, full_down, preferred_element_type=f32).astype(bf16),
            here,
            scatter_dimension=0,
            tiled=True,
        )
        gate_dots = jnp.sum((plain_act * raw_grad).reshape(-1, outer_count, part), axis=-1)
        lane = jnp.arange(INNER) == lax.axis_index("inner")
        gate_dots = jnp.where(lane[None, None, :], gate_dots[:, :, None], 0.0).reshape(-1, experts)
        gate_grads = lax.psum_scatter(gate_dots, here, scatter_dimension=0, tiled=True)
        gate_grad = (
            hidden_grad * up_act * sigmoid_gate * (1.0 + gate_act * (1.0 - sigmoid_gate))
        ).astype(bf16)
        up_grad = (hidden_grad * gate_act * sigmoid_gate).astype(bf16)
        copy_grads = (
            jnp.einsum("rf,df->rd", gate_grad, full_gate, preferred_element_type=f32)
            + jnp.einsum("rf,df->rd", up_grad, full_up, preferred_element_type=f32)
        ).astype(bf16)
        rows_back = lax.psum_scatter(copy_grads, here, scatter_dimension=0, tiled=True)
        down_w_grad = jnp.einsum("rf,rd->fd", hidden_act, rows_grad, preferred_element_type=f32)
        gate_w_grad = jnp.einsum("rd,rf->df", rows_in, gate_grad, preferred_element_type=f32)
        up_w_grad = jnp.einsum("rd,rf->df", rows_in, up_grad, preferred_element_type=f32)
        gate_w_grad, up_w_grad, down_w_grad = (
            lax.psum_scatter(gate_w_grad.astype(bf16), "outer", scatter_dimension=1, tiled=True),
            lax.psum_scatter(up_w_grad.astype(bf16), "outer", scatter_dimension=1, tiled=True),
            lax.psum_scatter(down_w_grad.astype(bf16), "outer", scatter_dimension=0, tiled=True),
        )
        gate_w_grad, up_w_grad, down_w_grad = (
            gate_w_grad[None].astype(f32),
            up_w_grad[None].astype(f32),
            down_w_grad[None].astype(f32),
        )
    cotangent = grad_out.astype(f32)
    logit_grads = (
        gate_probs * (gate_grads - jnp.sum(gate_probs * gate_grads, axis=-1, keepdims=True))
    ).astype(bf16)
    router_grad = jnp.einsum("sd,se->de", ffn_normed, logit_grads, preferred_element_type=f32)
    normed_two_grad = jnp.einsum("se,de->sd", logit_grads, router, preferred_element_type=f32)
    normed_two_grad = normed_two_grad + rows_back.astype(f32)
    mixed_part, ffn_gain_grad = norm_back(mixed_rows, scale_two, ffn_gain, normed_two_grad)
    mixed_grad = cotangent + mixed_part
    branch_grad = mixed_grad.astype(bf16)
    out_w_grad = jnp.einsum("sh,sd->hd", attended, branch_grad, preferred_element_type=f32)
    attended_grad = jnp.einsum("sd,hd->sh", branch_grad, w_out, preferred_element_type=f32).astype(
        bf16
    )
    attended_grad = attended_grad.reshape(length, kv_count, group_size, head_dim)
    scores = attention_probs(grouped, key_rows, allowed, head_dim)
    weights_prob = jnp.exp(scores - log_total)
    value_grad = jnp.einsum(
        "ngqk,qngd->knd", weights_prob.astype(bf16), attended_grad, preferred_element_type=f32
    )
    prob_grad = jnp.einsum("qngd,knd->ngqk", attended_grad, value_rows, preferred_element_type=f32)
    score_grad = (
        weights_prob * (prob_grad - jnp.sum(weights_prob * prob_grad, axis=-1, keepdims=True))
    ).astype(bf16)
    query_grad = jnp.einsum(
        "ngqk,knd->qngd", score_grad, key_rows, preferred_element_type=f32
    ) * head_dim ** (-0.5)
    key_grad = jnp.einsum(
        "ngqk,qngd->knd", score_grad, grouped, preferred_element_type=f32
    ) * head_dim ** (-0.5)
    query_grad = rotate(
        query_grad.reshape(length, head_count, head_dim), cosine_table, sine_table, -1.0
    )
    query_grad = query_grad.reshape(length, -1).astype(bf16)
    key_grad = rotate(key_grad, cosine_table, sine_table, -1.0).reshape(length, -1).astype(bf16)
    value_grad = value_grad.reshape(length, -1).astype(bf16)
    query_w_grad = jnp.einsum("sd,sh->dh", normed, query_grad, preferred_element_type=f32)
    key_w_grad = jnp.einsum("sd,sh->dh", normed, key_grad, preferred_element_type=f32)
    value_w_grad = jnp.einsum("sd,sh->dh", normed, value_grad, preferred_element_type=f32)
    normed_one_grad = (
        jnp.einsum("sh,dh->sd", query_grad, w_query, preferred_element_type=f32)
        + jnp.einsum("sh,dh->sd", key_grad, w_key, preferred_element_type=f32)
        + jnp.einsum("sh,dh->sd", value_grad, w_value, preferred_element_type=f32)
    )
    input_part, attn_gain_grad = norm_back(inputs, scale_one, attn_gain, normed_one_grad)
    grad_in = (mixed_grad + input_part).astype(bf16)
    everywhere = ("outer", "inner", "narrow")
    small = jnp.concatenate(
        [router_grad, attn_gain_grad[:, None], ffn_gain_grad[:, None]], axis=1
    )
    small = jnp.pad(small, ((0, 0), (0, 128 - small.shape[1])))
    if fused:
        turned = jnp.concatenate([query_grad, key_grad, value_grad], axis=1)
        mixed_late, turned = lax.optimization_barrier((mixed_rows, turned))
        hidden_out = (mixed_late + moe_rows.astype(f32)).astype(bf16)
        small, hidden_out, weight_last = lax.optimization_barrier(
            (small, hidden_out, weight_last)
        )
        weight_sum = weight_first.astype(f32) + weight_last.astype(f32)
        gate_w_grad = weight_sum[:part].T[None]
        up_w_grad = weight_sum[part : 2 * part].T[None]
        down_w_grad = weight_sum[2 * part :][None]
        out_sum, query_sum, key_sum, value_sum = reduce_layer(
            normed, turned, attended, branch_grad, small, outer_count
        )
        key_width = w_key.shape[1]
        small = value_sum[:, key_width:].astype(f32)
        summed = (
            small[:, experts],
            query_sum.astype(f32),
            key_sum.astype(f32),
            value_sum[:, :key_width].astype(f32),
            out_sum.astype(f32),
            small[:, experts + 1],
            small[:, :experts],
        )
    else:
        columns = jnp.concatenate(
            [query_w_grad, key_w_grad, value_w_grad, out_w_grad, small], axis=1
        ).astype(bf16)
        hidden_out = (mixed_rows + moe_rows.astype(f32)).astype(bf16)
        shares = lax.psum_scatter(columns, everywhere, scatter_dimension=0, tiled=True)
        columns = lax.all_gather(shares, everywhere, axis=0, tiled=True).astype(f32)
        starts = [0]
        for width in (w_query.shape[1], w_key.shape[1], w_value.shape[1], model_width, experts, 1, 1):
            starts.append(starts[-1] + width)
        pieces = [columns[:, low:high] for low, high in zip(starts[:-1], starts[1:])]
        summed = (
            pieces[5][:, 0],
            pieces[0],
            pieces[1],
            pieces[2],
            pieces[3],
            pieces[6][:, 0],
            pieces[4],
        )
    return (
        hidden_out,
        grad_in,
        summed[0],
        summed[1],
        summed[2],
        summed[3],
        summed[4],
        summed[5],
        summed[6],
        gate_w_grad,
        up_w_grad,
        down_w_grad,
    )


def solution(mesh):
    names = ("outer", "inner", "narrow")
    narrow = mesh.shape["narrow"]
    cut = Mesh(mesh.devices.reshape(-1, INNER, narrow), names)
    rows = P(names, None)
    columns = P(("outer", "inner"), None, "narrow")
    depths = P(("outer", "inner"), "narrow", None)
    return jax.shard_map(
        on_device,
        mesh=cut,
        in_specs=(rows, rows, rows) + (P(),) * 7 + (columns, columns, depths, rows),
        out_specs=(rows, rows) + (P(),) * 7 + (columns, columns, depths),
        check_vma=False,
    )
```

```python
import functools

import jax
import jax.numpy as jnp
from jax import lax
from jax.experimental import pallas as pl
from jax.experimental.pallas import tpu as pltpu
from jax.sharding import Mesh
from jax.sharding import PartitionSpec as P

HD = 64
INNER = 4


EPSILON = 1e-05


def norm_scale(values):
    return lax.rsqrt(jnp.mean(values * values, axis=-1, keepdims=True) + EPSILON)


def norm_back(values, inv_rms, gain_vector, grad_rows):
    weighted = grad_rows * gain_vector
    inner = jnp.mean(weighted * values, axis=-1, keepdims=True)
    value_grad = inv_rms * weighted - values * (inv_rms * inv_rms * inv_rms) * inner
    return (value_grad, jnp.sum(grad_rows * values * inv_rms, axis=0))


def rope_tables(length, head_dim):
    half_size = head_dim // 2
    freqs = 10000.0 ** (-(jnp.arange(half_size, dtype=jnp.float32) * 2.0) / head_dim)
    angles = jnp.arange(length, dtype=jnp.float32)[:, None] * freqs[None, :]
    return (jnp.cos(angles), jnp.sin(angles))


def rotate(values, cosine_table, sine_table, direction):
    half_size = values.shape[-1] // 2
    first_half = values[..., :half_size]
    second_half = values[..., half_size:]
    cosine_part = cosine_table[:, None, :]
    sine_part = sine_table[:, None, :] * direction
    return jnp.concatenate(
        [
            first_half * cosine_part - second_half * sine_part,
            second_half * cosine_part + first_half * sine_part,
        ],
        axis=-1,
    )


def attention_probs(grouped, key_rows, allowed, head_dim):
    scores = jnp.einsum(
        "qngd,knd->ngqk", grouped, key_rows, preferred_element_type=jnp.float32
    ) * head_dim ** (-0.5)
    return jnp.where(allowed, scores, -1e30)


def dot_nn(left, right):
    return lax.dot_general(left, right, (((1,), (0,)), ((), ())), preferred_element_type=jnp.float32)


def dot_nt(left, right):
    return lax.dot_general(left, right, (((1,), (1,)), ((), ())), preferred_element_type=jnp.float32)


def dot_tn(left, right):
    return lax.dot_general(left, right, (((0,), (0,)), ((), ())), preferred_element_type=jnp.float32)


def expert_kernel(
    outer_count,
    x_hbm,
    gate_hbm,
    grad_hbm,
    pair_own,
    down_own,
    pair_next,
    down_next,
    dx_hbm,
    y_hbm,
    dots_ref,
    first_hbm,
    last_hbm,
    rows,
    gates,
    act,
    both,
    wide,
    down,
    grads,
    total,
    stage_a,
    stage_b,
    ring,
    core_in,
    relay_in,
    last_in,
    dots,
    dots_in,
    local_sem,
    grad_sem,
    y_sem,
    gather_send,
    gather_recv,
    weight_send,
    weight_recv,
    ring_send,
    ring_recv,
    dots_send,
    dots_recv,
    back_send,
    back_recv,
):
    f32 = jnp.float32
    bf16 = jnp.bfloat16
    length, part = rows.shape[1], down.shape[1]
    half = length // 2
    outer, inner, narrow = lax.axis_index("outer"), lax.axis_index("inner"), lax.axis_index("narrow")
    side, core = inner // 2, inner % 2
    core_at = {"inner": side * 2 + (1 - core)}
    x_at = {"narrow": 1 - narrow}
    y_at = {"inner": (1 - side) * 2 + core}
    next_at = {"outer": lax.rem(outer + 1, outer_count)}
    before_at = {"outer": lax.rem(outer + outer_count - 1, outer_count)}

    def device_of(slot):
        there = slot // 2
        return {
            "inner": ((side + there // 2) % 2) * 2 + (core + slot % 2) % 2,
            "narrow": (narrow + there % 2) % 2,
        }

    def place_of(slot):
        there = slot // 2
        at_inner = ((side + there // 2) % 2) * 2 + (core + slot % 2) % 2
        return at_inner * 2 + (narrow + there % 2) % 2

    def remote(source, target, sends, recvs, index, device):
        return pltpu.make_async_remote_copy(
            src_ref=source,
            dst_ref=target,
            send_sem=sends.at[index],
            recv_sem=recvs.at[index],
            device_id=device,
            device_id_type=pl.DeviceIdType.MESH,
        )

    def local(source, target, index):
        return pltpu.make_async_copy(source, target, local_sem.at[index])

    low, high = pl.ds(0, half), pl.ds(half, half)
    dx_ref = total.at[pl.ds(0, length)]

    def gather(index):
        source, target, device = (
            (rows.at[0], rows.at[1], core_at),
            (rows.at[0], rows.at[2], x_at),
            (rows.at[0], rows.at[4], y_at),
            (rows.at[2, low], rows.at[6, low], y_at),
            (rows.at[4, high], rows.at[6, high], x_at),
            (rows.at[2], rows.at[3], core_at),
            (rows.at[4], rows.at[5], core_at),
            (rows.at[6], rows.at[7], core_at),
            (gates.at[0], gates.at[1], core_at),
            (gates.at[0], gates.at[2], x_at),
            (gates.at[0], gates.at[4], y_at),
            (gates.at[0], gates.at[6], device_of(6)),
            (gates.at[2], gates.at[3], core_at),
            (gates.at[4], gates.at[5], core_at),
            (gates.at[6], gates.at[7], core_at),
        )[index]
        return remote(source, target, gather_send, gather_recv, index, device)

    def wide_at(slot):
        return wide.at[:, pl.ds(slot * 2 * part, 2 * part)]

    def weight(index):
        source, target, device = ((1, 2, next_at), (0, 3, before_at))[index // 2]
        if index % 2 == 0:
            return remote(
                wide_at(source), wide_at(target), weight_send, weight_recv, index, device
            )
        return remote(
            down.at[source], down.at[target], weight_send, weight_recv, index, device
        )

    def ring_copy(index):
        source = (stage_a, stage_b)[index]
        return remote(source, ring.at[index], ring_send, ring_recv, index, next_at)

    def dots_copy(slot):
        return remote(
            dots.at[slot], dots_in.at[slot], dots_send, dots_recv, slot, device_of(slot)
        )

    def back(index):
        source, target, device = (
            (rows.at[1], core_in.at[0], core_at),
            (rows.at[3], core_in.at[1], core_at),
            (rows.at[5], core_in.at[2], core_at),
            (rows.at[7], core_in.at[3], core_at),
            (rows.at[6, low], relay_in.at[0], x_at),
            (rows.at[6, high], relay_in.at[1], y_at),
            (rows.at[2], last_in.at[0], x_at),
            (rows.at[4], last_in.at[1], y_at),
        )[index]
        return remote(source, target, back_send, back_recv, index, device)

    own_copies = (
        local(x_hbm, rows.at[0], 0),
        local(gate_hbm, gates.at[0], 1),
        local(pair_next, wide_at(1), 2),
        local(down_next, down.at[1], 3),
        local(pair_own, wide_at(0), 4),
        local(down_own, down.at[0], 5),
    )
    for copy in own_copies:
        copy.start()

    def fetch(step):
        order = step % 8
        slot = jnp.where(order == 3, 4, jnp.where(order == 4, 3, order))
        return pltpu.make_async_copy(
            grad_hbm.at[place_of(slot)], grads.at[step % 2], grad_sem.at[step % 2]
        )

    fetch(0).start()
    barrier = pltpu.get_barrier_semaphore()
    for slot in range(1, 8):
        pl.semaphore_signal(
            barrier, inc=1, device_id=device_of(slot), device_id_type=pl.DeviceIdType.MESH
        )
    for device in (next_at, before_at):
        pl.semaphore_signal(
            barrier, inc=1, device_id=device, device_id_type=pl.DeviceIdType.MESH
        )
    pl.semaphore_wait(barrier, 9)
    own_copies[0].wait()
    own_copies[1].wait()
    for index in (1, 2, 9, 10, 11, 0, 8):
        gather(index).start()
    for copy in own_copies[2:]:
        copy.wait()
    weight(0).start()
    weight(1).start()

    def first_step(step, carry):
        turn, order = step // 8, step % 8
        slot = jnp.where(order == 3, 4, jnp.where(order == 4, 3, order))
        block = jnp.where(turn == 0, 1, jnp.where(turn == 1, 2, jnp.where(turn == 2, 0, 3)))

        @pl.when(step + 1 < 8 * outer_count)
        def _():
            fetch(step + 1).start()

        @pl.when(step == 1)
        def _():
            gather(0).wait_recv()
            gather(8).wait_recv()

        @pl.when(step == 2)
        def _():
            gather(1).wait_recv()
            gather(3).start()
            gather(5).start()
            gather(2).wait_recv()
            gather(4).start()
            gather(6).start()
            gather(9).wait_recv()
            gather(12).start()
            gather(10).wait_recv()
            gather(13).start()

        @pl.when(step == 4)
        def _():
            gather(5).wait_recv()
            gather(12).wait_recv()

        @pl.when(step == 5)
        def _():
            gather(6).wait_recv()
            gather(13).wait_recv()

        @pl.when(step == 6)
        def _():
            gather(3).wait_recv()
            gather(4).wait_recv()
            gather(7).start()
            gather(11).wait_recv()
            gather(14).start()

        @pl.when(step == 7)
        def _():
            gather(7).wait_recv()
            gather(14).wait_recv()

        @pl.when(step == 8)
        def _():
            weight(0).wait_recv()
            weight(1).wait_recv()
            weight(2).start()
            weight(3).start()

        @pl.when(step == 20)
        def _():
            weight(2).wait_recv()
            weight(3).wait_recv()
            ring_copy(0).start()

        fetch(step).wait()
        here = rows[slot]
        grad_rows = grads[step % 2]
        products = dot_nn(here, wide[:, pl.ds(block * 2 * part, 2 * part)])
        gate_act, up_act = products[:, :part], products[:, part:]
        raw = dot_nt(grad_rows, down[block])
        expert = lax.rem(outer + outer_count - block, outer_count) * INNER + inner
        count = gates.shape[1] // 3
        place = lax.broadcasted_iota(jnp.int32, (gates.shape[1], part), 0) % count
        chosen = jnp.where(place == expert, 1.0, 0.0).astype(bf16)
        weights = dot_tn(gates[slot], chosen)
        sigmoid = 1.0 / (1.0 + jnp.exp(-gate_act))
        silu = gate_act * sigmoid
        plain = silu * up_act
        act[slot, :, pl.ds(block * part, part)] = (weights * plain).astype(bf16)
        products = (plain * raw).astype(bf16)
        dots[slot, pl.ds(block, 1), :] = dot_nt(jnp.ones((8, part), bf16), products)[:1]
        hidden = weights * raw
        both[slot, :, pl.ds(block * 2 * part, part)] = (
            hidden * up_act * sigmoid * (1.0 + gate_act * (1.0 - sigmoid))
        ).astype(bf16)
        both[slot, :, pl.ds(block * 2 * part + part, part)] = (hidden * silu).astype(bf16)
        pair_grad = dot_tn(both[slot, :, pl.ds(block * 2 * part, 2 * part)], here)
        down_grad = dot_tn(act[slot, :, pl.ds(block * part, part)], grad_rows)

        total[: 2 * part] = jnp.where(order == 0, pair_grad, total[: 2 * part] + pair_grad)
        total[2 * part :] = jnp.where(order == 0, down_grad, total[2 * part :] + down_grad)

        @pl.when(step == 7)
        def _():
            stage_a[...] = total[...].astype(bf16)

        @pl.when(step == 15)
        def _():
            stage_b[...] = total[...].astype(bf16)

        @pl.when(step == 23)
        def _():
            copy = local(total, first_hbm, 0)
            copy.start()
            copy.wait()

        return carry

    lax.fori_loop(0, 8 * outer_count, first_step, 0)
    ring_copy(0).wait()
    stage_a[...] = total[...].astype(bf16)
    stage_b[...] = (stage_b[...].astype(f32) + ring[0].astype(f32)).astype(bf16)
    ring_copy(1).start()
    for slot in range(1, 8):
        dots_copy(slot).start()
    for index in range(15):
        gather(index).wait_send()

    def second_step(order, carry):
        turn = order // 2
        there = jnp.where(turn == 0, 3, jnp.where(turn == 3, 0, turn))
        slot = there * 2 + 1 - order % 2
        dx_ref[...] = dot_nt(both[slot], wide[...])

        @pl.when(order % 2 == 0)
        def _():
            rows[slot] = dx_ref[...].astype(bf16)

        for index in range(4):

            @pl.when((order % 2 == 0) & (there == index))
            def _():
                back(index).start()

        @pl.when(order == 1)
        def _():
            back(3).wait_recv()
            rows[6] = (dx_ref[...] + core_in[3].astype(f32)).astype(bf16)
            back(4).start()
            back(5).start()

        @pl.when(order == 3)
        def _():
            back(1).wait_recv()
            back(5).wait_recv()
            rows[2, :half] = (dx_ref[:half] + core_in[1, :half].astype(f32)).astype(bf16)
            rows[2, half:] = (
                dx_ref[half:] + core_in[1, half:].astype(f32) + relay_in[1].astype(f32)
            ).astype(bf16)
            back(6).start()

        @pl.when(order == 5)
        def _():
            back(2).wait_recv()
            back(4).wait_recv()
            rows[4, :half] = (
                dx_ref[:half] + core_in[2, :half].astype(f32) + relay_in[0].astype(f32)
            ).astype(bf16)
            rows[4, half:] = (dx_ref[half:] + core_in[2, half:].astype(f32)).astype(bf16)
            back(7).start()

        return carry

    lax.fori_loop(0, 8, second_step, 0)

    def third_step(slot, carry):
        act[slot] = dot_nn(act[slot], down[...].reshape(outer_count * part, -1)).astype(bf16)
        pltpu.make_async_copy(act.at[slot], y_hbm.at[place_of(slot)], y_sem.at[slot]).start()
        return carry

    lax.fori_loop(0, 8, third_step, 0)
    ring_copy(1).wait()
    stage_a[...] = (stage_a[...].astype(f32) + ring[1].astype(f32)).astype(bf16)
    local(stage_a, last_hbm, 0).start()
    back(0).wait_recv()
    back(6).wait_recv()
    back(7).wait_recv()
    dx_ref[...] = (
        dx_ref[...]
        + core_in[0].astype(f32)
        + (last_in[0].astype(f32) + last_in[1].astype(f32))
    )
    local(dx_ref, dx_hbm, 1).start()
    dots_ref[0] = dots[0]
    for slot in range(1, 8):
        dots_copy(slot).wait()
        dots_ref[slot] = dots_in[slot]
    for index in range(8):
        back(index).wait_send()
    for index in range(4):
        weight(index).wait_send()
    for slot in range(8):
        pltpu.make_async_copy(act.at[slot], y_hbm.at[place_of(slot)], y_sem.at[slot]).wait()
    local(stage_a, last_hbm, 0).wait()
    local(dx_ref, dx_hbm, 1).wait()


def expert_layer(rows_own, gate_table, rows_grad, pair_own, down_own, outer_count):
    f32 = jnp.float32
    bf16 = jnp.bfloat16
    length, width = rows_own.shape
    part = down_own.shape[0]
    ahead = [(place, (place + 1) % outer_count) for place in range(outer_count)]
    pair_next = lax.ppermute(pair_own, "outer", ahead)
    down_next = lax.ppermute(down_own, "outer", ahead)
    anywhere = pl.BlockSpec(memory_space=pl.ANY)
    inside = pl.BlockSpec(memory_space=pltpu.VMEM)
    vmem, dma = pltpu.VMEM, pltpu.SemaphoreType.DMA
    hidden = outer_count * part
    share = jax.ShapeDtypeStruct((3 * part, width), bf16)
    dx, y_rows, dots, first, last = pl.pallas_call(
        functools.partial(expert_kernel, outer_count),
        out_shape=(
            jax.ShapeDtypeStruct((length, width), f32),
            jax.ShapeDtypeStruct((8, length, width), bf16),
            jax.ShapeDtypeStruct((8, 8, length), f32),
            jax.ShapeDtypeStruct((3 * part, width), f32),
            share,
        ),
        in_specs=[anywhere] * 7,
        out_specs=(anywhere, anywhere, inside, anywhere, anywhere),
        scratch_shapes=[
            vmem((8, length, width), bf16),
            vmem((8,) + gate_table.shape, bf16),
            vmem((8, length, hidden), bf16),
            vmem((8, length, 2 * hidden), bf16),
            vmem((width, 2 * hidden), bf16),
            vmem((outer_count, part, width), bf16),
            vmem((2, length, width), bf16),
            vmem((3 * part, width), f32),
            vmem((3 * part, width), bf16),
            vmem((3 * part, width), bf16),
            vmem((2, 3 * part, width), bf16),
            vmem((4, length, width), bf16),
            vmem((2, length // 2, width), bf16),
            vmem((2, length, width), bf16),
            vmem((8, 8, length), f32),
            vmem((8, 8, length), f32),
            dma((6,)),
            dma((2,)),
            dma((8,)),
            dma((15,)),
            dma((15,)),
            dma((4,)),
            dma((4,)),
            dma((2,)),
            dma((2,)),
            dma((8,)),
            dma((8,)),
            dma((8,)),
            dma((8,)),
        ],
        compiler_params=pltpu.CompilerParams(
            collective_id=0, has_side_effects=True, vmem_limit_bytes=67043328
        ),
        cost_estimate=pl.CostEstimate(
            flops=18 * 8 * length * width * hidden, bytes_accessed=1 << 26, transcendentals=0
        ),
        name="expert_layer",
    )(
        rows_own,
        gate_table,
        rows_grad.reshape(8, length, width),
        pair_own,
        down_own,
        pair_next,
        down_next,
    )
    last = lax.ppermute(last, "outer", ahead)
    return dx, y_rows.reshape(8 * length, width), dots, first, last


def reduce_kernel(
    outer_count,
    normed_ref,
    turned_ref,
    attended_ref,
    branch_ref,
    small_ref,
    out_one,
    out_two,
    out_three,
    out_four,
    work_one,
    work_two,
    work_three,
    work_four,
    core_one,
    core_two,
    core_three,
    core_four,
    near_one,
    near_two,
    near_three,
    near_four,
    far_one,
    far_two,
    far_three,
    far_four,
    deep_one,
    deep_two,
    deep_three,
    deep_four,
    sends,
    recvs,
    deep_sends,
    deep_recvs,
):
    f32 = jnp.float32
    bf16 = jnp.bfloat16
    outer, inner, narrow = lax.axis_index("outer"), lax.axis_index("inner"), lax.axis_index("narrow")
    side, core = inner // 2, inner % 2
    core_at = {"inner": side * 2 + (1 - core)}
    x_at = {"narrow": 1 - narrow}
    y_at = {"inner": (1 - side) * 2 + core}
    outs = (out_one, out_two, out_three, out_four)
    works = (work_one, work_two, work_three, work_four)
    cores = (core_one, core_two, core_three, core_four)
    nears = (near_one, near_two, near_three, near_four)
    fars = (far_one, far_two, far_three, far_four)
    deeps = (deep_one, deep_two, deep_three, deep_four)
    rows = work_one.shape[0]
    halves, quarters, eighths = rows // 2, rows // 4, rows // 8
    pieces = eighths // outer_count

    def span(start, size):
        return pl.ds(pl.multiple_of(start, pieces), size)

    def remote(source, target, chunk, stage, device):
        return pltpu.make_async_remote_copy(
            src_ref=source,
            dst_ref=target,
            send_sem=sends.at[chunk * 8 + stage],
            recv_sem=recvs.at[chunk * 8 + stage],
            device_id=device,
            device_id_type=pl.DeviceIdType.MESH,
        )

    def places(chunk):
        first, second = (narrow, side) if chunk % 2 == 0 else (side, narrow)
        devices = (x_at, y_at) if chunk % 2 == 0 else (y_at, x_at)
        at_core = core * halves
        at_near = at_core + first * quarters
        at_far = at_near + second * eighths
        return first, second, devices, at_core, at_near, at_far

    def copies(chunk, stage):
        first, second, devices, at_core, at_near, at_far = places(chunk)
        work, out = works[chunk], outs[chunk]
        if stage == 0:
            source = work.at[span((1 - core) * halves, halves)]
            return [remote(source, cores[chunk], chunk, 0, core_at)]
        if stage == 1:
            source = work.at[span(at_core + (1 - first) * quarters, quarters)]
            return [remote(source, nears[chunk], chunk, 1, devices[0])]
        if stage == 2:
            source = work.at[span(at_near + (1 - second) * eighths, eighths)]
            return [remote(source, fars[chunk], chunk, 2, devices[1])]
        if stage in (3, 4):
            found = []
            for step in range(1, outer_count):
                there = lax.rem(outer + step, outer_count)
                index = (chunk * 2 + stage - 3) * (outer_count - 1) + step - 1
                if stage == 3:
                    source = work.at[span(at_far + there * pieces, pieces)]
                    target = deeps[chunk].at[step - 1]
                else:
                    source = out.at[span(at_far + outer * pieces, pieces)]
                    target = source
                found.append(
                    pltpu.make_async_remote_copy(
                        src_ref=source,
                        dst_ref=target,
                        send_sem=deep_sends.at[index],
                        recv_sem=deep_recvs.at[index],
                        device_id={"outer": there},
                        device_id_type=pl.DeviceIdType.MESH,
                    )
                )
            return found
        start, size, device = (
            (at_far, eighths, devices[1]),
            (at_near, quarters, devices[0]),
            (at_core, halves, core_at),
        )[stage - 5]
        source = out.at[span(start, size)]
        return [remote(source, source, chunk, stage, device)]

    def arrive(chunk, stage):
        first, second, devices, at_core, at_near, at_far = places(chunk)
        work, out = works[chunk], outs[chunk]
        for copy in copies(chunk, stage):
            copy.wait_recv()
        if stage < 3:
            start, size, box = (
                (at_core, halves, cores[chunk]),
                (at_near, quarters, nears[chunk]),
                (at_far, eighths, fars[chunk]),
            )[stage]
            held = work[span(start, size)].astype(f32) + box[...].astype(f32)
            work[span(start, size)] = held.astype(bf16)
        elif stage == 3:
            held = work[span(at_far + outer * pieces, pieces)].astype(f32)
            for step in range(outer_count - 1):
                held = held + deeps[chunk][step].astype(f32)
            out[span(at_far + outer * pieces, pieces)] = held.astype(bf16)

    barrier = pltpu.get_barrier_semaphore()
    others = [core_at, x_at, y_at]
    for step in range(1, outer_count):
        others.append({"outer": lax.rem(outer + step, outer_count)})
    for device in others:
        pl.semaphore_signal(
            barrier, inc=1, device_id=device, device_id_type=pl.DeviceIdType.MESH
        )
    width = small_ref.shape[1]
    model = normed_ref.shape[1]
    heads = attended_ref.shape[1]
    kept = (turned_ref.shape[1] - heads) // 2

    def product(chunk):
        if chunk == 0:
            work_one[...] = dot_tn(attended_ref[...], branch_ref[...]).astype(bf16)
        elif chunk == 1:
            work_two[...] = dot_tn(normed_ref[...], turned_ref[:, :heads]).astype(bf16)
        elif chunk == 2:
            work_three[...] = dot_tn(
                normed_ref[...], turned_ref[:, heads : heads + kept]
            ).astype(bf16)
        else:
            work_four[:, :kept] = dot_tn(
                normed_ref[...], turned_ref[:, heads + kept :]
            ).astype(bf16)
            work_four[:, kept:] = small_ref[...].astype(bf16)

    product(0)
    pl.semaphore_wait(barrier, 2 + outer_count)
    for slot in range(8 + 2):
        for chunk in range(4):
            stage = slot - chunk // 2
            if 0 < stage <= 8:
                arrive(chunk, stage - 1)
            if stage == 0 and chunk > 0:
                product(chunk)
            if 0 <= stage < 8:
                for copy in copies(chunk, stage):
                    copy.start()
    for chunk in range(4):
        for stage in range(8):
            for copy in copies(chunk, stage):
                copy.wait_send()


def reduce_layer(normed, turned, attended, branch, small, outer_count):
    bf16 = jnp.bfloat16
    model, heads = normed.shape[1], attended.shape[1]
    kept = (turned.shape[1] - heads) // 2
    tops = [heads, model, model, model]
    widths = [model, heads, kept, kept + small.shape[1]]
    vmem, dma = pltpu.VMEM, pltpu.SemaphoreType.DMA
    inside = pl.BlockSpec(memory_space=pltpu.VMEM)
    scratch = []
    for cut in (1, 2, 4, 8):
        scratch += [vmem((top // cut, width), bf16) for top, width in zip(tops, widths)]
    scratch += [
        vmem((outer_count - 1, top // 8 // outer_count, width), bf16)
        for top, width in zip(tops, widths)
    ]
    return pl.pallas_call(
        functools.partial(reduce_kernel, outer_count),
        out_shape=tuple(
            jax.ShapeDtypeStruct((top, width), bf16) for top, width in zip(tops, widths)
        ),
        in_specs=[inside] * 5,
        out_specs=(inside,) * 4,
        scratch_shapes=scratch
        + [dma((32,)), dma((32,)), dma((8 * (outer_count - 1),)), dma((8 * (outer_count - 1),))],
        compiler_params=pltpu.CompilerParams(
            collective_id=1, has_side_effects=True, vmem_limit_bytes=60 << 20
        ),
        name="reduce_layer",
    )(normed, turned, attended, branch, small)


def on_device(
    hidden_in,
    segment_ids,
    expert_ids,
    attn_gain,
    w_query,
    w_key,
    w_value,
    w_out,
    ffn_gain,
    router,
    w_gate,
    w_up,
    w_down,
    grad_out,
):
    f32 = jnp.float32
    bf16 = jnp.bfloat16
    length, model_width = hidden_in.shape
    head_dim = HD
    head_count = w_query.shape[1] // head_dim
    kv_count = w_key.shape[1] // head_dim
    group_size = head_count // kv_count
    experts = router.shape[1]
    outer_count = experts // INNER
    here = ("inner", "narrow")
    fused = outer_count == 4 and lax.axis_size("narrow") == 2
    rows_grad = lax.all_gather(grad_out, here, axis=0, tiled=True)
    part = w_gate.shape[2]
    inputs = hidden_in.astype(f32)
    scale_one = norm_scale(inputs)
    normed = (inputs * scale_one * attn_gain).astype(bf16)
    query_pre = jnp.dot(normed, w_query, preferred_element_type=f32)
    key_pre = jnp.dot(normed, w_key, preferred_element_type=f32)
    value_pre = jnp.dot(normed, w_value, preferred_element_type=f32)
    cosine_table, sine_table = rope_tables(length, head_dim)
    query_rows = rotate(
        query_pre.reshape(length, head_count, head_dim), cosine_table, sine_table, 1.0
    ).astype(bf16)
    key_rows = rotate(
        key_pre.reshape(length, kv_count, head_dim), cosine_table, sine_table, 1.0
    ).astype(bf16)
    value_rows = value_pre.astype(bf16).reshape(length, kv_count, head_dim)
    grouped = query_rows.reshape(length, kv_count, group_size, head_dim)
    segments = segment_ids[0]
    places = jnp.arange(length, dtype=jnp.int32)
    allowed = (segments[:, None] == segments[None, :]) & (places[:, None] >= places[None, :])
    scores = attention_probs(grouped, key_rows, allowed, head_dim)
    row_max = jnp.max(scores, axis=-1, keepdims=True)
    log_total = row_max + jnp.log(jnp.sum(jnp.exp(scores - row_max), axis=-1, keepdims=True))
    weights_prob = jnp.exp(scores - log_total)
    attended = jnp.einsum(
        "ngqk,knd->qngd", weights_prob.astype(bf16), value_rows, preferred_element_type=f32
    )
    attended = attended.reshape(length, head_count * head_dim).astype(bf16)
    mixed_rows = inputs + jnp.dot(attended, w_out, preferred_element_type=f32)
    scale_two = norm_scale(mixed_rows)
    ffn_normed = (mixed_rows * scale_two * ffn_gain).astype(bf16)
    logits = jnp.dot(ffn_normed, router, preferred_element_type=f32)
    picked = expert_ids[:, :, None] == jnp.arange(experts, dtype=jnp.int32)[None, None, :]
    member = jnp.any(picked, axis=1)
    masked = jnp.where(member, logits, -jnp.inf)
    powers = jnp.where(member, jnp.exp(masked - jnp.max(masked, axis=-1, keepdims=True)), 0.0)
    gate_probs = powers / jnp.sum(powers, axis=-1, keepdims=True)
    if fused:
        table = gate_probs.T
        part_one = lax.reduce_precision(table, 8, 7)
        part_two = lax.reduce_precision(table - part_one, 8, 7)
        part_three = table - part_one - part_two
        table = jnp.concatenate([part_one, part_two, part_three], axis=0).astype(bf16)
        pair_own = jnp.concatenate([w_gate[0], w_up[0]], axis=1)
        rows_back, y_rows, dots, weight_first, weight_last = expert_layer(
            ffn_normed, table, rows_grad, pair_own, w_down[0], outer_count
        )
        moe_rows = lax.psum_scatter(y_rows, here, scatter_dimension=0, tiled=True)
        dots = dots[:, :outer_count].reshape(2, 2, 2, outer_count, length).sum(axis=1)
        each = jnp.arange(experts, dtype=jnp.int32)
        outer, inner = lax.axis_index("outer"), lax.axis_index("inner")
        side = (each % INNER // 2 + inner // 2) % 2
        core = (each + inner) % 2
        block = (outer + outer_count - each // INNER) % outer_count
        gate_grads = dots.reshape(experts, length)[(side * 2 + core) * outer_count + block].T
    else:
        full_gate = lax.all_gather(w_gate[0], "outer", axis=1, tiled=True)
        full_up = lax.all_gather(w_up[0], "outer", axis=1, tiled=True)
        full_down = lax.all_gather(w_down[0], "outer", axis=0, tiled=True)
        gate_table = lax.all_gather(gate_probs.T, here, axis=0, tiled=False)
        gate_table = gate_table.reshape(-1, outer_count, INNER, length)
        mine = lax.dynamic_index_in_dim(gate_table, lax.axis_index("inner"), 2, keepdims=False)
        row_gates = mine.transpose(0, 2, 1).reshape(-1, outer_count)
        gate_wide = jnp.repeat(row_gates, part, axis=1)
        rows_in = lax.all_gather(ffn_normed, here, axis=0, tiled=True)
        gate_act = jnp.dot(rows_in, full_gate, preferred_element_type=f32)
        up_act = jnp.dot(rows_in, full_up, preferred_element_type=f32)
        raw_grad = jnp.einsum("rd,fd->rf", rows_grad, full_down, preferred_element_type=f32)
        sigmoid_gate = jax.nn.sigmoid(gate_act)
        plain_act = gate_act * sigmoid_gate * up_act
        hidden_act = (gate_wide * plain_act).astype(bf16)
        hidden_grad = gate_wide * raw_grad
        moe_rows = lax.psum_scatter(
            jnp.dot(hidden_act, full_down, preferred_element_type=f32).astype(bf16),
            here,
            scatter_dimension=0,
            tiled=True,
        )
        gate_dots = jnp.sum((plain_act * raw_grad).reshape(-1, outer_count, part), axis=-1)
        lane = jnp.arange(INNER) == lax.axis_index("inner")
        gate_dots = jnp.where(lane[None, None, :], gate_dots[:, :, None], 0.0).reshape(-1, experts)
        gate_grads = lax.psum_scatter(gate_dots, here, scatter_dimension=0, tiled=True)
        gate_grad = (
            hidden_grad * up_act * sigmoid_gate * (1.0 + gate_act * (1.0 - sigmoid_gate))
        ).astype(bf16)
        up_grad = (hidden_grad * gate_act * sigmoid_gate).astype(bf16)
        copy_grads = (
            jnp.einsum("rf,df->rd", gate_grad, full_gate, preferred_element_type=f32)
            + jnp.einsum("rf,df->rd", up_grad, full_up, preferred_element_type=f32)
        ).astype(bf16)
        rows_back = lax.psum_scatter(copy_grads, here, scatter_dimension=0, tiled=True)
        down_w_grad = jnp.einsum("rf,rd->fd", hidden_act, rows_grad, preferred_element_type=f32)
        gate_w_grad = jnp.einsum("rd,rf->df", rows_in, gate_grad, preferred_element_type=f32)
        up_w_grad = jnp.einsum("rd,rf->df", rows_in, up_grad, preferred_element_type=f32)
        gate_w_grad, up_w_grad, down_w_grad = (
            lax.psum_scatter(gate_w_grad.astype(bf16), "outer", scatter_dimension=1, tiled=True),
            lax.psum_scatter(up_w_grad.astype(bf16), "outer", scatter_dimension=1, tiled=True),
            lax.psum_scatter(down_w_grad.astype(bf16), "outer", scatter_dimension=0, tiled=True),
        )
        gate_w_grad, up_w_grad, down_w_grad = (
            gate_w_grad[None].astype(f32),
            up_w_grad[None].astype(f32),
            down_w_grad[None].astype(f32),
        )
    cotangent = grad_out.astype(f32)
    logit_grads = (
        gate_probs * (gate_grads - jnp.sum(gate_probs * gate_grads, axis=-1, keepdims=True))
    ).astype(bf16)
    router_grad = jnp.einsum("sd,se->de", ffn_normed, logit_grads, preferred_element_type=f32)
    normed_two_grad = jnp.einsum("se,de->sd", logit_grads, router, preferred_element_type=f32)
    normed_two_grad = normed_two_grad + rows_back.astype(f32)
    mixed_part, ffn_gain_grad = norm_back(mixed_rows, scale_two, ffn_gain, normed_two_grad)
    mixed_grad = cotangent + mixed_part
    branch_grad = mixed_grad.astype(bf16)
    out_w_grad = jnp.einsum("sh,sd->hd", attended, branch_grad, preferred_element_type=f32)
    attended_grad = jnp.einsum("sd,hd->sh", branch_grad, w_out, preferred_element_type=f32).astype(
        bf16
    )
    attended_grad = attended_grad.reshape(length, kv_count, group_size, head_dim)
    scores = attention_probs(grouped, key_rows, allowed, head_dim)
    weights_prob = jnp.exp(scores - log_total)
    value_grad = jnp.einsum(
        "ngqk,qngd->knd", weights_prob.astype(bf16), attended_grad, preferred_element_type=f32
    )
    prob_grad = jnp.einsum("qngd,knd->ngqk", attended_grad, value_rows, preferred_element_type=f32)
    score_grad = (
        weights_prob * (prob_grad - jnp.sum(weights_prob * prob_grad, axis=-1, keepdims=True))
    ).astype(bf16)
    query_grad = jnp.einsum(
        "ngqk,knd->qngd", score_grad, key_rows, preferred_element_type=f32
    ) * head_dim ** (-0.5)
    key_grad = jnp.einsum(
        "ngqk,qngd->knd", score_grad, grouped, preferred_element_type=f32
    ) * head_dim ** (-0.5)
    query_grad = rotate(
        query_grad.reshape(length, head_count, head_dim), cosine_table, sine_table, -1.0
    )
    query_grad = query_grad.reshape(length, -1).astype(bf16)
    key_grad = rotate(key_grad, cosine_table, sine_table, -1.0).reshape(length, -1).astype(bf16)
    value_grad = value_grad.reshape(length, -1).astype(bf16)
    query_w_grad = jnp.einsum("sd,sh->dh", normed, query_grad, preferred_element_type=f32)
    key_w_grad = jnp.einsum("sd,sh->dh", normed, key_grad, preferred_element_type=f32)
    value_w_grad = jnp.einsum("sd,sh->dh", normed, value_grad, preferred_element_type=f32)
    normed_one_grad = (
        jnp.einsum("sh,dh->sd", query_grad, w_query, preferred_element_type=f32)
        + jnp.einsum("sh,dh->sd", key_grad, w_key, preferred_element_type=f32)
        + jnp.einsum("sh,dh->sd", value_grad, w_value, preferred_element_type=f32)
    )
    input_part, attn_gain_grad = norm_back(inputs, scale_one, attn_gain, normed_one_grad)
    grad_in = (mixed_grad + input_part).astype(bf16)
    everywhere = ("outer", "inner", "narrow")
    small = jnp.concatenate(
        [router_grad, attn_gain_grad[:, None], ffn_gain_grad[:, None]], axis=1
    )
    small = jnp.pad(small, ((0, 0), (0, 128 - small.shape[1])))
    if fused:
        turned = jnp.concatenate([query_grad, key_grad, value_grad], axis=1)
        mixed_late, turned = lax.optimization_barrier((mixed_rows, turned))
        hidden_out = (mixed_late + moe_rows.astype(f32)).astype(bf16)
        small, hidden_out, weight_last = lax.optimization_barrier(
            (small, hidden_out, weight_last)
        )
        weight_sum = weight_first + weight_last.astype(f32)
        gate_w_grad = weight_sum[:part].T[None]
        up_w_grad = weight_sum[part : 2 * part].T[None]
        down_w_grad = weight_sum[2 * part :][None]
        out_sum, query_sum, key_sum, value_sum = reduce_layer(
            normed, turned, attended, branch_grad, small, outer_count
        )
        key_width = w_key.shape[1]
        small = value_sum[:, key_width:].astype(f32)
        summed = (
            small[:, experts],
            query_sum.astype(f32),
            key_sum.astype(f32),
            value_sum[:, :key_width].astype(f32),
            out_sum.astype(f32),
            small[:, experts + 1],
            small[:, :experts],
        )
    else:
        columns = jnp.concatenate(
            [query_w_grad, key_w_grad, value_w_grad, out_w_grad, small], axis=1
        ).astype(bf16)
        hidden_out = (mixed_rows + moe_rows.astype(f32)).astype(bf16)
        shares = lax.psum_scatter(columns, everywhere, scatter_dimension=0, tiled=True)
        columns = lax.all_gather(shares, everywhere, axis=0, tiled=True).astype(f32)
        starts = [0]
        for width in (w_query.shape[1], w_key.shape[1], w_value.shape[1], model_width, experts, 1, 1):
            starts.append(starts[-1] + width)
        pieces = [columns[:, low:high] for low, high in zip(starts[:-1], starts[1:])]
        summed = (
            pieces[5][:, 0],
            pieces[0],
            pieces[1],
            pieces[2],
            pieces[3],
            pieces[6][:, 0],
            pieces[4],
        )
    return (
        hidden_out,
        grad_in,
        summed[0],
        summed[1],
        summed[2],
        summed[3],
        summed[4],
        summed[5],
        summed[6],
        gate_w_grad,
        up_w_grad,
        down_w_grad,
    )


def solution(mesh):
    names = ("outer", "inner", "narrow")
    narrow = mesh.shape["narrow"]
    cut = Mesh(mesh.devices.reshape(-1, INNER, narrow), names)
    rows = P(names, None)
    columns = P(("outer", "inner"), None, "narrow")
    depths = P(("outer", "inner"), "narrow", None)
    return jax.shard_map(
        on_device,
        mesh=cut,
        in_specs=(rows, rows, rows) + (P(),) * 7 + (columns, columns, depths, rows),
        out_specs=(rows, rows) + (P(),) * 7 + (columns, columns, depths),
        check_vma=False,
    )
```

```python
import functools

import jax
import jax.numpy as jnp
from jax import lax
from jax.experimental import pallas as pl
from jax.experimental.pallas import tpu as pltpu
from jax.sharding import Mesh
from jax.sharding import PartitionSpec as P

HD = 64
INNER = 4


EPSILON = 1e-05


def norm_scale(values):
    return lax.rsqrt(jnp.mean(values * values, axis=-1, keepdims=True) + EPSILON)


def norm_back(values, inv_rms, gain_vector, grad_rows):
    weighted = grad_rows * gain_vector
    inner = jnp.mean(weighted * values, axis=-1, keepdims=True)
    value_grad = inv_rms * weighted - values * (inv_rms * inv_rms * inv_rms) * inner
    return (value_grad, jnp.sum(grad_rows * values * inv_rms, axis=0))


def rope_tables(length, head_dim):
    half_size = head_dim // 2
    freqs = 10000.0 ** (-(jnp.arange(half_size, dtype=jnp.float32) * 2.0) / head_dim)
    angles = jnp.arange(length, dtype=jnp.float32)[:, None] * freqs[None, :]
    return (jnp.cos(angles), jnp.sin(angles))


def rotate(values, cosine_table, sine_table, direction):
    half_size = values.shape[-1] // 2
    first_half = values[..., :half_size]
    second_half = values[..., half_size:]
    cosine_part = cosine_table[:, None, :]
    sine_part = sine_table[:, None, :] * direction
    return jnp.concatenate(
        [
            first_half * cosine_part - second_half * sine_part,
            second_half * cosine_part + first_half * sine_part,
        ],
        axis=-1,
    )


def attention_probs(grouped, key_rows, allowed, head_dim):
    scores = jnp.einsum(
        "qngd,knd->ngqk", grouped, key_rows, preferred_element_type=jnp.float32
    ) * head_dim ** (-0.5)
    return jnp.where(allowed, scores, -1e30)


def dot_nn(left, right):
    return lax.dot_general(left, right, (((1,), (0,)), ((), ())), preferred_element_type=jnp.float32)


def dot_nt(left, right):
    return lax.dot_general(left, right, (((1,), (1,)), ((), ())), preferred_element_type=jnp.float32)


def dot_tn(left, right):
    return lax.dot_general(left, right, (((0,), (0,)), ((), ())), preferred_element_type=jnp.float32)


def expert_kernel(
    outer_count,
    x_hbm,
    gate_hbm,
    grad_own,
    grad_x,
    grad_y,
    grad_far,
    pair_own,
    down_own,
    pair_next,
    down_next,
    dx_hbm,
    y_hbm,
    dots_ref,
    first_hbm,
    last_hbm,
    grad_other,
    ring_hbm,
    rows,
    gates,
    act,
    both,
    wide,
    down,
    grads,
    total,
    stage_a,
    stage_b,
    ring,
    core_in,
    relay_in,
    last_in,
    dots,
    dots_in,
    local_sem,
    grad_sem,
    y_sem,
    gather_send,
    gather_recv,
    weight_send,
    weight_recv,
    ring_send,
    ring_recv,
    dots_send,
    dots_recv,
    back_send,
    back_recv,
    swap_send,
    swap_recv,
):
    f32 = jnp.float32
    bf16 = jnp.bfloat16
    length, part = rows.shape[1], down.shape[1]
    half = length // 2
    outer, inner, narrow = lax.axis_index("outer"), lax.axis_index("inner"), lax.axis_index("narrow")
    side, core = inner // 2, inner % 2
    core_at = {"inner": side * 2 + (1 - core)}
    x_at = {"narrow": 1 - narrow}
    y_at = {"inner": (1 - side) * 2 + core}
    next_at = {"outer": lax.rem(outer + 1, outer_count)}
    before_at = {"outer": lax.rem(outer + outer_count - 1, outer_count)}

    def device_of(slot):
        there = slot // 2
        return {
            "inner": ((side + there // 2) % 2) * 2 + (core + slot % 2) % 2,
            "narrow": (narrow + there % 2) % 2,
        }

    def place_of(slot):
        there = slot // 2
        at_inner = ((side + there // 2) % 2) * 2 + (core + slot % 2) % 2
        return at_inner * 2 + (narrow + there % 2) % 2

    def remote(source, target, sends, recvs, index, device):
        return pltpu.make_async_remote_copy(
            src_ref=source,
            dst_ref=target,
            send_sem=sends.at[index],
            recv_sem=recvs.at[index],
            device_id=device,
            device_id_type=pl.DeviceIdType.MESH,
        )

    def local(source, target, index):
        return pltpu.make_async_copy(source, target, local_sem.at[index])

    low, high = pl.ds(0, half), pl.ds(half, half)
    dx_ref = total.at[pl.ds(0, length)]

    def gather(index):
        source, target, device = (
            (rows.at[0], rows.at[1], core_at),
            (rows.at[0], rows.at[2], x_at),
            (rows.at[0], rows.at[4], y_at),
            (rows.at[2, low], rows.at[6, low], y_at),
            (rows.at[4, high], rows.at[6, high], x_at),
            (rows.at[2], rows.at[3], core_at),
            (rows.at[4], rows.at[5], core_at),
            (rows.at[6], rows.at[7], core_at),
            (gates.at[0], gates.at[1], core_at),
            (gates.at[0], gates.at[2], x_at),
            (gates.at[0], gates.at[4], y_at),
            (gates.at[0], gates.at[6], device_of(6)),
            (gates.at[2], gates.at[3], core_at),
            (gates.at[4], gates.at[5], core_at),
            (gates.at[6], gates.at[7], core_at),
        )[index]
        return remote(source, target, gather_send, gather_recv, index, device)

    def wide_at(slot):
        return wide.at[:, pl.ds(slot * 2 * part, 2 * part)]

    def weight(index):
        source, target, device = ((1, 2, next_at), (0, 3, before_at))[index // 2]
        if index % 2 == 0:
            return remote(
                wide_at(source), wide_at(target), weight_send, weight_recv, index, device
            )
        return remote(
            down.at[source], down.at[target], weight_send, weight_recv, index, device
        )

    def ring_copy(index):
        source, target = ((stage_a, ring), (stage_b, ring_hbm))[index]
        return remote(source, target, ring_send, ring_recv, index, next_at)

    def dots_copy(slot):
        return remote(
            dots.at[slot], dots_in.at[slot], dots_send, dots_recv, slot, device_of(slot)
        )

    def back(index):
        source, target, device = (
            (rows.at[1], core_in.at[0], core_at),
            (rows.at[3], core_in.at[1], core_at),
            (rows.at[5], core_in.at[2], core_at),
            (rows.at[7], core_in.at[3], core_at),
            (rows.at[6, low], relay_in.at[0], x_at),
            (rows.at[6, high], relay_in.at[1], y_at),
            (rows.at[2], last_in.at[0], x_at),
            (rows.at[4], last_in.at[1], y_at),
        )[index]
        return remote(source, target, back_send, back_recv, index, device)

    own_copies = (
        local(x_hbm, rows.at[0], 0),
        local(gate_hbm, gates.at[0], 1),
        local(pair_next, wide_at(1), 2),
        local(down_next, down.at[1], 3),
        local(pair_own, wide_at(0), 4),
        local(down_own, down.at[0], 5),
    )
    for copy in own_copies:
        copy.start()

    grad_same = (grad_own, grad_x, grad_y, grad_far)

    def swap(index):
        return remote(
            grad_same[index], grad_other.at[index], swap_send, swap_recv, index, core_at
        )

    def slot_at(step):
        order = step % 8
        return jnp.where(order == 3, 4, jnp.where(order == 4, 3, order))

    def fetch_from(source, step):
        return pltpu.make_async_copy(source, grads.at[step % 2], grad_sem.at[step % 2])

    def fetch(step):
        slot = slot_at(step)
        for index in range(4):

            @pl.when(slot == 2 * index)
            def _():
                fetch_from(grad_same[index], step).start()

        @pl.when(slot % 2 == 1)
        def _():
            fetch_from(grad_other.at[slot // 2], step).start()

    fetch_from(grad_own, 0).start()
    barrier = pltpu.get_barrier_semaphore()
    for slot in range(1, 8):
        pl.semaphore_signal(
            barrier, inc=1, device_id=device_of(slot), device_id_type=pl.DeviceIdType.MESH
        )
    for device in (next_at, before_at):
        pl.semaphore_signal(
            barrier, inc=1, device_id=device, device_id_type=pl.DeviceIdType.MESH
        )
    pl.semaphore_wait(barrier, 9)
    own_copies[0].wait()
    own_copies[1].wait()
    for index in (1, 2, 9, 10, 11, 0, 8):
        gather(index).start()
    for copy in own_copies[2:]:
        copy.wait()
    weight(0).start()
    weight(1).start()
    for index in range(4):
        swap(index).start()

    def forward(slot, block, grad_rows):
        products = dot_nn(rows[slot], wide[:, pl.ds(block * 2 * part, 2 * part)])
        gate_act, up_act = products[:, :part], products[:, part:]
        raw = dot_nt(grad_rows, down[block])
        expert = lax.rem(outer + outer_count - block, outer_count) * INNER + inner
        count = gates.shape[1] // 3
        place = lax.broadcasted_iota(jnp.int32, (gates.shape[1], part), 0) % count
        chosen = jnp.where(place == expert, 1.0, 0.0).astype(bf16)
        weights = dot_tn(gates[slot], chosen)
        sigmoid = 1.0 / (1.0 + jnp.exp(-gate_act))
        silu = gate_act * sigmoid
        plain = silu * up_act
        act[slot, :, pl.ds(block * part, part)] = (weights * plain).astype(bf16)
        products = (plain * raw).astype(bf16)
        dots[slot, pl.ds(block, 1), :] = dot_nt(jnp.ones((8, part), bf16), products)[:1]
        hidden = weights * raw
        both[slot, :, pl.ds(block * 2 * part, part)] = (
            hidden * up_act * sigmoid * (1.0 + gate_act * (1.0 - sigmoid))
        ).astype(bf16)
        both[slot, :, pl.ds(block * 2 * part + part, part)] = (hidden * silu).astype(bf16)

    def gather_weights(slot, block, order, grad_rows):
        pair_grad = dot_tn(both[slot, :, pl.ds(block * 2 * part, 2 * part)], rows[slot])
        down_grad = dot_tn(act[slot, :, pl.ds(block * part, part)], grad_rows)
        total[: 2 * part] = jnp.where(order == 0, pair_grad, total[: 2 * part] + pair_grad)
        total[2 * part :] = jnp.where(order == 0, down_grad, total[2 * part :] + down_grad)

    def open_step(step, carry):
        slot = slot_at(step)

        @pl.when(step == 0)
        def _():
            swap(0).wait_recv()

        @pl.when(step == 1)
        def _():
            gather(0).wait_recv()
            gather(8).wait_recv()

        @pl.when(step == 2)
        def _():
            gather(1).wait_recv()
            gather(3).start()
            gather(5).start()
            gather(2).wait_recv()
            gather(4).start()
            gather(6).start()
            gather(9).wait_recv()
            gather(12).start()
            gather(10).wait_recv()
            gather(13).start()

        @pl.when(step == 3)
        def _():
            swap(1).wait_recv()

        @pl.when(step == 4)
        def _():
            gather(5).wait_recv()
            gather(12).wait_recv()
            swap(2).wait_recv()

        @pl.when(step == 5)
        def _():
            weight(2).start()
            weight(3).start()
            gather(6).wait_recv()
            gather(13).wait_recv()

        @pl.when(step == 6)
        def _():
            swap(3).wait_recv()
            gather(3).wait_recv()
            gather(4).wait_recv()
            gather(7).start()
            gather(11).wait_recv()
            gather(14).start()

        @pl.when(step == 7)
        def _():
            gather(7).wait_recv()
            gather(14).wait_recv()

        fetch(step + 1)
        fetch_from(grad_own, step).wait()
        grad_rows = grads[step % 2]
        forward(slot, 1, grad_rows)
        forward(slot, 0, grad_rows)
        gather_weights(slot, 1, step, grad_rows)
        return carry

    def first_step(step, carry):
        turn, order = step // 8, step % 8
        slot = slot_at(step)
        block = jnp.where(turn == 1, 2, jnp.where(turn == 2, 0, 3))

        @pl.when(step + 1 < 8 * outer_count)
        def _():
            fetch(step + 1)

        @pl.when(step == 20)
        def _():
            weight(2).wait_recv()
            weight(3).wait_recv()
            ring_copy(0).start()

        fetch_from(grad_own, step).wait()
        grad_rows = grads[step % 2]

        @pl.when(turn != 2)
        def _():
            forward(slot, block, grad_rows)

        gather_weights(slot, block, order, grad_rows)

        @pl.when(step == 15)
        def _():
            stage_b[...] = total[...].astype(bf16)

        @pl.when(step == 23)
        def _():
            copy = local(total, first_hbm, 0)
            copy.start()
            copy.wait()

        return carry

    lax.fori_loop(0, 8, open_step, 0)
    stage_a[...] = total[...].astype(bf16)
    weight(0).wait_recv()
    weight(1).wait_recv()
    lax.fori_loop(8, 8 * outer_count, first_step, 0)
    ring_copy(0).wait()
    stage_a[...] = total[...].astype(bf16)
    stage_b[...] = (stage_b[...].astype(f32) + ring[...].astype(f32)).astype(bf16)
    ring_copy(1).start()
    for slot in range(1, 8):
        dots_copy(slot).start()
    for index in range(15):
        gather(index).wait_send()

    def second_step(order, carry):
        slot = jnp.where(order < 2, 7 - order, jnp.where(order > 5, 7 - order, 0))
        for index, found in ((2, 3), (3, 5), (4, 2), (5, 4)):
            slot = jnp.where(order == index, found, slot)
        dx_ref[...] = dot_nt(both[slot], wide[...])

        @pl.when(slot % 2 == 1)
        def _():
            rows[slot] = dx_ref[...].astype(bf16)

        for index in range(4):

            @pl.when(slot == 2 * index + 1)
            def _():
                back(index).start()

        @pl.when(slot == 6)
        def _():
            back(3).wait_recv()
            rows[6] = (dx_ref[...] + core_in[3].astype(f32)).astype(bf16)
            back(4).start()
            back(5).start()

        @pl.when(slot == 2)
        def _():
            back(1).wait_recv()
            back(5).wait_recv()
            rows[2, :half] = (dx_ref[:half] + core_in[1, :half].astype(f32)).astype(bf16)
            rows[2, half:] = (
                dx_ref[half:] + core_in[1, half:].astype(f32) + relay_in[1].astype(f32)
            ).astype(bf16)
            back(6).start()

        @pl.when(slot == 4)
        def _():
            back(2).wait_recv()
            back(4).wait_recv()
            rows[4, :half] = (
                dx_ref[:half] + core_in[2, :half].astype(f32) + relay_in[0].astype(f32)
            ).astype(bf16)
            rows[4, half:] = (dx_ref[half:] + core_in[2, half:].astype(f32)).astype(bf16)
            back(7).start()

        return carry

    lax.fori_loop(0, 8, second_step, 0)

    def third_step(slot, carry):
        act[slot] = dot_nn(act[slot], down[...].reshape(outer_count * part, -1)).astype(bf16)
        pltpu.make_async_copy(act.at[slot], y_hbm.at[place_of(slot)], y_sem.at[slot]).start()
        return carry

    lax.fori_loop(0, 8, third_step, 0)
    ring_copy(1).wait()
    arrived = local(ring_hbm, ring, 2)
    arrived.start()
    arrived.wait()
    stage_a[...] = (stage_a[...].astype(f32) + ring[...].astype(f32)).astype(bf16)
    local(stage_a, last_hbm, 0).start()
    back(0).wait_recv()
    back(6).wait_recv()
    back(7).wait_recv()
    dx_ref[...] = (
        dx_ref[...]
        + core_in[0].astype(f32)
        + (last_in[0].astype(f32) + last_in[1].astype(f32))
    )
    local(dx_ref, dx_hbm, 1).start()
    dots_ref[0] = dots[0]
    for slot in range(1, 8):
        dots_copy(slot).wait()
        dots_ref[slot] = dots_in[slot]
    for index in range(8):
        back(index).wait_send()
    for index in range(4):
        weight(index).wait_send()
        swap(index).wait_send()
    for slot in range(8):
        pltpu.make_async_copy(act.at[slot], y_hbm.at[place_of(slot)], y_sem.at[slot]).wait()
    local(stage_a, last_hbm, 0).wait()
    local(dx_ref, dx_hbm, 1).wait()


def expert_layer(rows_own, gate_table, grad_own, pair_own, down_own, outer_count):
    f32 = jnp.float32
    bf16 = jnp.bfloat16
    length, width = rows_own.shape
    part = down_own.shape[0]
    ahead = [(place, (place + 1) % outer_count) for place in range(outer_count)]
    grad_x = lax.ppermute(grad_own, "narrow", [(0, 1), (1, 0)])
    grad_y = lax.ppermute(grad_own, "inner", [(place, (place + 2) % 4) for place in range(4)])
    across = [(place, (place // 2 + 2) % 4 * 2 + 1 - place % 2) for place in range(8)]
    grad_far = lax.ppermute(grad_own, ("inner", "narrow"), across)
    pair_next = lax.ppermute(pair_own, "outer", ahead)
    down_next = lax.ppermute(down_own, "outer", ahead)
    anywhere = pl.BlockSpec(memory_space=pl.ANY)
    inside = pl.BlockSpec(memory_space=pltpu.VMEM)
    vmem, dma = pltpu.VMEM, pltpu.SemaphoreType.DMA
    hidden = outer_count * part
    share = jax.ShapeDtypeStruct((3 * part, width), bf16)
    dx, y_rows, dots, first, last, _, _ = pl.pallas_call(
        functools.partial(expert_kernel, outer_count),
        out_shape=(
            jax.ShapeDtypeStruct((length, width), f32),
            jax.ShapeDtypeStruct((8, length, width), bf16),
            jax.ShapeDtypeStruct((8, 8, length), f32),
            jax.ShapeDtypeStruct((3 * part, width), f32),
            share,
            jax.ShapeDtypeStruct((4, length, width), bf16),
            share,
        ),
        in_specs=[anywhere] * 10,
        out_specs=(anywhere, anywhere, inside, anywhere, anywhere, anywhere, anywhere),
        scratch_shapes=[
            vmem((8, length, width), bf16),
            vmem((8,) + gate_table.shape, bf16),
            vmem((8, length, hidden), bf16),
            vmem((8, length, 2 * hidden), bf16),
            vmem((width, 2 * hidden), bf16),
            vmem((outer_count, part, width), bf16),
            vmem((2, length, width), bf16),
            vmem((3 * part, width), f32),
            vmem((3 * part, width), bf16),
            vmem((3 * part, width), bf16),
            vmem((3 * part, width), bf16),
            vmem((4, length, width), bf16),
            vmem((2, length // 2, width), bf16),
            vmem((2, length, width), bf16),
            vmem((8, 8, length), f32),
            vmem((8, 8, length), f32),
            dma((6,)),
            dma((2,)),
            dma((8,)),
            dma((15,)),
            dma((15,)),
            dma((4,)),
            dma((4,)),
            dma((2,)),
            dma((2,)),
            dma((8,)),
            dma((8,)),
            dma((8,)),
            dma((8,)),
            dma((4,)),
            dma((4,)),
        ],
        compiler_params=pltpu.CompilerParams(
            collective_id=0, has_side_effects=True, vmem_limit_bytes=67043328
        ),
        cost_estimate=pl.CostEstimate(
            flops=18 * 8 * length * width * hidden, bytes_accessed=1 << 26, transcendentals=0
        ),
        name="expert_layer",
    )(
        rows_own,
        gate_table,
        grad_own,
        grad_x,
        grad_y,
        grad_far,
        pair_own,
        down_own,
        pair_next,
        down_next,
    )
    last = lax.ppermute(last, "outer", ahead)
    return dx, y_rows.reshape(8 * length, width), dots, first, last


def reduce_kernel(
    outer_count,
    normed_ref,
    turned_ref,
    attended_ref,
    branch_ref,
    small_ref,
    out_one,
    out_two,
    out_three,
    out_four,
    work_one,
    work_two,
    work_three,
    work_four,
    core_one,
    core_two,
    core_three,
    core_four,
    near_one,
    near_two,
    near_three,
    near_four,
    far_one,
    far_two,
    far_three,
    far_four,
    deep_one,
    deep_two,
    deep_three,
    deep_four,
    sends,
    recvs,
    deep_sends,
    deep_recvs,
):
    f32 = jnp.float32
    bf16 = jnp.bfloat16
    outer, inner, narrow = lax.axis_index("outer"), lax.axis_index("inner"), lax.axis_index("narrow")
    side, core = inner // 2, inner % 2
    core_at = {"inner": side * 2 + (1 - core)}
    x_at = {"narrow": 1 - narrow}
    y_at = {"inner": (1 - side) * 2 + core}
    outs = (out_one, out_two, out_three, out_four)
    works = (work_one, work_two, work_three, work_four)
    cores = (core_one, core_two, core_three, core_four)
    nears = (near_one, near_two, near_three, near_four)
    fars = (far_one, far_two, far_three, far_four)
    deeps = (deep_one, deep_two, deep_three, deep_four)
    rows = work_one.shape[0]
    halves, quarters, eighths = rows // 2, rows // 4, rows // 8
    pieces = eighths // outer_count

    def span(start, size):
        return pl.ds(pl.multiple_of(start, pieces), size)

    def remote(source, target, chunk, stage, device):
        return pltpu.make_async_remote_copy(
            src_ref=source,
            dst_ref=target,
            send_sem=sends.at[chunk * 8 + stage],
            recv_sem=recvs.at[chunk * 8 + stage],
            device_id=device,
            device_id_type=pl.DeviceIdType.MESH,
        )

    def places(chunk):
        first, second = (narrow, side) if chunk % 2 == 0 else (side, narrow)
        devices = (x_at, y_at) if chunk % 2 == 0 else (y_at, x_at)
        at_core = core * halves
        at_near = at_core + first * quarters
        at_far = at_near + second * eighths
        return first, second, devices, at_core, at_near, at_far

    def copies(chunk, stage):
        first, second, devices, at_core, at_near, at_far = places(chunk)
        work, out = works[chunk], outs[chunk]
        if stage == 0:
            source = work.at[span((1 - core) * halves, halves)]
            return [remote(source, cores[chunk], chunk, 0, core_at)]
        if stage == 1:
            source = work.at[span(at_core + (1 - first) * quarters, quarters)]
            return [remote(source, nears[chunk], chunk, 1, devices[0])]
        if stage == 2:
            source = work.at[span(at_near + (1 - second) * eighths, eighths)]
            return [remote(source, fars[chunk], chunk, 2, devices[1])]
        if stage in (3, 4):
            found = []
            for step in range(1, outer_count):
                there = lax.rem(outer + step, outer_count)
                index = (chunk * 2 + stage - 3) * (outer_count - 1) + step - 1
                if stage == 3:
                    source = work.at[span(at_far + there * pieces, pieces)]
                    target = deeps[chunk].at[step - 1]
                else:
                    source = out.at[span(at_far + outer * pieces, pieces)]
                    target = source
                found.append(
                    pltpu.make_async_remote_copy(
                        src_ref=source,
                        dst_ref=target,
                        send_sem=deep_sends.at[index],
                        recv_sem=deep_recvs.at[index],
                        device_id={"outer": there},
                        device_id_type=pl.DeviceIdType.MESH,
                    )
                )
            return found
        start, size, device = (
            (at_far, eighths, devices[1]),
            (at_near, quarters, devices[0]),
            (at_core, halves, core_at),
        )[stage - 5]
        source = out.at[span(start, size)]
        return [remote(source, source, chunk, stage, device)]

    def arrive(chunk, stage):
        first, second, devices, at_core, at_near, at_far = places(chunk)
        work, out = works[chunk], outs[chunk]
        for copy in copies(chunk, stage):
            copy.wait_recv()
        if stage < 3:
            start, size, box = (
                (at_core, halves, cores[chunk]),
                (at_near, quarters, nears[chunk]),
                (at_far, eighths, fars[chunk]),
            )[stage]
            held = work[span(start, size)].astype(f32) + box[...].astype(f32)
            work[span(start, size)] = held.astype(bf16)
        elif stage == 3:
            held = work[span(at_far + outer * pieces, pieces)].astype(f32)
            for step in range(outer_count - 1):
                held = held + deeps[chunk][step].astype(f32)
            out[span(at_far + outer * pieces, pieces)] = held.astype(bf16)

    barrier = pltpu.get_barrier_semaphore()
    others = [core_at, x_at, y_at]
    for step in range(1, outer_count):
        others.append({"outer": lax.rem(outer + step, outer_count)})
    for device in others:
        pl.semaphore_signal(
            barrier, inc=1, device_id=device, device_id_type=pl.DeviceIdType.MESH
        )
    width = small_ref.shape[1]
    model = normed_ref.shape[1]
    heads = attended_ref.shape[1]
    kept = (turned_ref.shape[1] - heads) // 2

    def product(chunk):
        if chunk == 0:
            work_one[...] = dot_tn(attended_ref[...], branch_ref[...]).astype(bf16)
        elif chunk == 1:
            work_two[...] = dot_tn(normed_ref[...], turned_ref[:, :heads]).astype(bf16)
        elif chunk == 2:
            work_three[...] = dot_tn(
                normed_ref[...], turned_ref[:, heads : heads + kept]
            ).astype(bf16)
        else:
            work_four[:, :kept] = dot_tn(
                normed_ref[...], turned_ref[:, heads + kept :]
            ).astype(bf16)
            work_four[:, kept:] = small_ref[...].astype(bf16)

    product(0)
    pl.semaphore_wait(barrier, 2 + outer_count)
    for slot in range(8 + 2):
        for chunk in range(4):
            stage = slot - chunk // 2
            if 0 < stage <= 8:
                arrive(chunk, stage - 1)
            if stage == 0 and chunk > 0:
                product(chunk)
            if 0 <= stage < 8:
                for copy in copies(chunk, stage):
                    copy.start()
    for chunk in range(4):
        for stage in range(8):
            for copy in copies(chunk, stage):
                copy.wait_send()


def reduce_layer(normed, turned, attended, branch, small, outer_count):
    bf16 = jnp.bfloat16
    model, heads = normed.shape[1], attended.shape[1]
    kept = (turned.shape[1] - heads) // 2
    tops = [heads, model, model, model]
    widths = [model, heads, kept, kept + small.shape[1]]
    vmem, dma = pltpu.VMEM, pltpu.SemaphoreType.DMA
    inside = pl.BlockSpec(memory_space=pltpu.VMEM)
    scratch = []
    for cut in (1, 2, 4, 8):
        scratch += [vmem((top // cut, width), bf16) for top, width in zip(tops, widths)]
    scratch += [
        vmem((outer_count - 1, top // 8 // outer_count, width), bf16)
        for top, width in zip(tops, widths)
    ]
    return pl.pallas_call(
        functools.partial(reduce_kernel, outer_count),
        out_shape=tuple(
            jax.ShapeDtypeStruct((top, width), bf16) for top, width in zip(tops, widths)
        ),
        in_specs=[inside] * 5,
        out_specs=(inside,) * 4,
        scratch_shapes=scratch
        + [dma((32,)), dma((32,)), dma((8 * (outer_count - 1),)), dma((8 * (outer_count - 1),))],
        compiler_params=pltpu.CompilerParams(
            collective_id=1, has_side_effects=True, vmem_limit_bytes=60 << 20
        ),
        name="reduce_layer",
    )(normed, turned, attended, branch, small)


def on_device(
    hidden_in,
    segment_ids,
    expert_ids,
    attn_gain,
    w_query,
    w_key,
    w_value,
    w_out,
    ffn_gain,
    router,
    w_gate,
    w_up,
    w_down,
    grad_out,
):
    f32 = jnp.float32
    bf16 = jnp.bfloat16
    length, model_width = hidden_in.shape
    head_dim = HD
    head_count = w_query.shape[1] // head_dim
    kv_count = w_key.shape[1] // head_dim
    group_size = head_count // kv_count
    experts = router.shape[1]
    outer_count = experts // INNER
    here = ("inner", "narrow")
    fused = outer_count == 4 and lax.axis_size("narrow") == 2
    part = w_gate.shape[2]
    inputs = hidden_in.astype(f32)
    scale_one = norm_scale(inputs)
    normed = (inputs * scale_one * attn_gain).astype(bf16)
    query_pre = jnp.dot(normed, w_query, preferred_element_type=f32)
    key_pre = jnp.dot(normed, w_key, preferred_element_type=f32)
    value_pre = jnp.dot(normed, w_value, preferred_element_type=f32)
    cosine_table, sine_table = rope_tables(length, head_dim)
    query_rows = rotate(
        query_pre.reshape(length, head_count, head_dim), cosine_table, sine_table, 1.0
    ).astype(bf16)
    key_rows = rotate(
        key_pre.reshape(length, kv_count, head_dim), cosine_table, sine_table, 1.0
    ).astype(bf16)
    value_rows = value_pre.astype(bf16).reshape(length, kv_count, head_dim)
    grouped = query_rows.reshape(length, kv_count, group_size, head_dim)
    segments = segment_ids[0]
    places = jnp.arange(length, dtype=jnp.int32)
    allowed = (segments[:, None] == segments[None, :]) & (places[:, None] >= places[None, :])
    scores = attention_probs(grouped, key_rows, allowed, head_dim)
    row_max = jnp.max(scores, axis=-1, keepdims=True)
    log_total = row_max + jnp.log(jnp.sum(jnp.exp(scores - row_max), axis=-1, keepdims=True))
    weights_prob = jnp.exp(scores - log_total)
    attended = jnp.einsum(
        "ngqk,knd->qngd", weights_prob.astype(bf16), value_rows, preferred_element_type=f32
    )
    attended = attended.reshape(length, head_count * head_dim).astype(bf16)
    mixed_rows = inputs + jnp.dot(attended, w_out, preferred_element_type=f32)
    scale_two = norm_scale(mixed_rows)
    ffn_normed = (mixed_rows * scale_two * ffn_gain).astype(bf16)
    logits = jnp.dot(ffn_normed, router, preferred_element_type=f32)
    picked = expert_ids[:, :, None] == jnp.arange(experts, dtype=jnp.int32)[None, None, :]
    member = jnp.any(picked, axis=1)
    masked = jnp.where(member, logits, -jnp.inf)
    powers = jnp.where(member, jnp.exp(masked - jnp.max(masked, axis=-1, keepdims=True)), 0.0)
    gate_probs = powers / jnp.sum(powers, axis=-1, keepdims=True)
    if fused:
        table = gate_probs.T
        part_one = lax.reduce_precision(table, 8, 7)
        part_two = lax.reduce_precision(table - part_one, 8, 7)
        part_three = table - part_one - part_two
        table = jnp.concatenate([part_one, part_two, part_three], axis=0).astype(bf16)
        pair_own = jnp.concatenate([w_gate[0], w_up[0]], axis=1)
        rows_back, y_rows, dots, weight_first, weight_last = expert_layer(
            ffn_normed, table, grad_out, pair_own, w_down[0], outer_count
        )
        moe_rows = lax.psum_scatter(y_rows, here, scatter_dimension=0, tiled=True)
        dots = dots[:, :outer_count].reshape(2, 2, 2, outer_count, length).sum(axis=1)
        each = jnp.arange(experts, dtype=jnp.int32)
        outer, inner = lax.axis_index("outer"), lax.axis_index("inner")
        side = (each % INNER // 2 + inner // 2) % 2
        core = (each + inner) % 2
        block = (outer + outer_count - each // INNER) % outer_count
        gate_grads = dots.reshape(experts, length)[(side * 2 + core) * outer_count + block].T
    else:
        rows_grad = lax.all_gather(grad_out, here, axis=0, tiled=True)
        full_gate = lax.all_gather(w_gate[0], "outer", axis=1, tiled=True)
        full_up = lax.all_gather(w_up[0], "outer", axis=1, tiled=True)
        full_down = lax.all_gather(w_down[0], "outer", axis=0, tiled=True)
        gate_table = lax.all_gather(gate_probs.T, here, axis=0, tiled=False)
        gate_table = gate_table.reshape(-1, outer_count, INNER, length)
        mine = lax.dynamic_index_in_dim(gate_table, lax.axis_index("inner"), 2, keepdims=False)
        row_gates = mine.transpose(0, 2, 1).reshape(-1, outer_count)
        gate_wide = jnp.repeat(row_gates, part, axis=1)
        rows_in = lax.all_gather(ffn_normed, here, axis=0, tiled=True)
        gate_act = jnp.dot(rows_in, full_gate, preferred_element_type=f32)
        up_act = jnp.dot(rows_in, full_up, preferred_element_type=f32)
        raw_grad = jnp.einsum("rd,fd->rf", rows_grad, full_down, preferred_element_type=f32)
        sigmoid_gate = jax.nn.sigmoid(gate_act)
        plain_act = gate_act * sigmoid_gate * up_act
        hidden_act = (gate_wide * plain_act).astype(bf16)
        hidden_grad = gate_wide * raw_grad
        moe_rows = lax.psum_scatter(
            jnp.dot(hidden_act, full_down, preferred_element_type=f32).astype(bf16),
            here,
            scatter_dimension=0,
            tiled=True,
        )
        gate_dots = jnp.sum((plain_act * raw_grad).reshape(-1, outer_count, part), axis=-1)
        lane = jnp.arange(INNER) == lax.axis_index("inner")
        gate_dots = jnp.where(lane[None, None, :], gate_dots[:, :, None], 0.0).reshape(-1, experts)
        gate_grads = lax.psum_scatter(gate_dots, here, scatter_dimension=0, tiled=True)
        gate_grad = (
            hidden_grad * up_act * sigmoid_gate * (1.0 + gate_act * (1.0 - sigmoid_gate))
        ).astype(bf16)
        up_grad = (hidden_grad * gate_act * sigmoid_gate).astype(bf16)
        copy_grads = (
            jnp.einsum("rf,df->rd", gate_grad, full_gate, preferred_element_type=f32)
            + jnp.einsum("rf,df->rd", up_grad, full_up, preferred_element_type=f32)
        ).astype(bf16)
        rows_back = lax.psum_scatter(copy_grads, here, scatter_dimension=0, tiled=True)
        down_w_grad = jnp.einsum("rf,rd->fd", hidden_act, rows_grad, preferred_element_type=f32)
        gate_w_grad = jnp.einsum("rd,rf->df", rows_in, gate_grad, preferred_element_type=f32)
        up_w_grad = jnp.einsum("rd,rf->df", rows_in, up_grad, preferred_element_type=f32)
        gate_w_grad, up_w_grad, down_w_grad = (
            lax.psum_scatter(gate_w_grad.astype(bf16), "outer", scatter_dimension=1, tiled=True),
            lax.psum_scatter(up_w_grad.astype(bf16), "outer", scatter_dimension=1, tiled=True),
            lax.psum_scatter(down_w_grad.astype(bf16), "outer", scatter_dimension=0, tiled=True),
        )
        gate_w_grad, up_w_grad, down_w_grad = (
            gate_w_grad[None].astype(f32),
            up_w_grad[None].astype(f32),
            down_w_grad[None].astype(f32),
        )
    cotangent = grad_out.astype(f32)
    logit_grads = (
        gate_probs * (gate_grads - jnp.sum(gate_probs * gate_grads, axis=-1, keepdims=True))
    ).astype(bf16)
    router_grad = jnp.einsum("sd,se->de", ffn_normed, logit_grads, preferred_element_type=f32)
    normed_two_grad = jnp.einsum("se,de->sd", logit_grads, router, preferred_element_type=f32)
    normed_two_grad = normed_two_grad + rows_back.astype(f32)
    mixed_part, ffn_gain_grad = norm_back(mixed_rows, scale_two, ffn_gain, normed_two_grad)
    mixed_grad = cotangent + mixed_part
    branch_grad = mixed_grad.astype(bf16)
    out_w_grad = jnp.einsum("sh,sd->hd", attended, branch_grad, preferred_element_type=f32)
    attended_grad = jnp.einsum("sd,hd->sh", branch_grad, w_out, preferred_element_type=f32).astype(
        bf16
    )
    attended_grad = attended_grad.reshape(length, kv_count, group_size, head_dim)
    scores = attention_probs(grouped, key_rows, allowed, head_dim)
    weights_prob = jnp.exp(scores - log_total)
    value_grad = jnp.einsum(
        "ngqk,qngd->knd", weights_prob.astype(bf16), attended_grad, preferred_element_type=f32
    )
    prob_grad = jnp.einsum("qngd,knd->ngqk", attended_grad, value_rows, preferred_element_type=f32)
    score_grad = (
        weights_prob * (prob_grad - jnp.sum(weights_prob * prob_grad, axis=-1, keepdims=True))
    ).astype(bf16)
    query_grad = jnp.einsum(
        "ngqk,knd->qngd", score_grad, key_rows, preferred_element_type=f32
    ) * head_dim ** (-0.5)
    key_grad = jnp.einsum(
        "ngqk,qngd->knd", score_grad, grouped, preferred_element_type=f32
    ) * head_dim ** (-0.5)
    query_grad = rotate(
        query_grad.reshape(length, head_count, head_dim), cosine_table, sine_table, -1.0
    )
    query_grad = query_grad.reshape(length, -1).astype(bf16)
    key_grad = rotate(key_grad, cosine_table, sine_table, -1.0).reshape(length, -1).astype(bf16)
    value_grad = value_grad.reshape(length, -1).astype(bf16)
    query_w_grad = jnp.einsum("sd,sh->dh", normed, query_grad, preferred_element_type=f32)
    key_w_grad = jnp.einsum("sd,sh->dh", normed, key_grad, preferred_element_type=f32)
    value_w_grad = jnp.einsum("sd,sh->dh", normed, value_grad, preferred_element_type=f32)
    normed_one_grad = (
        jnp.einsum("sh,dh->sd", query_grad, w_query, preferred_element_type=f32)
        + jnp.einsum("sh,dh->sd", key_grad, w_key, preferred_element_type=f32)
        + jnp.einsum("sh,dh->sd", value_grad, w_value, preferred_element_type=f32)
    )
    input_part, attn_gain_grad = norm_back(inputs, scale_one, attn_gain, normed_one_grad)
    grad_in = (mixed_grad + input_part).astype(bf16)
    everywhere = ("outer", "inner", "narrow")
    small = jnp.concatenate(
        [router_grad, attn_gain_grad[:, None], ffn_gain_grad[:, None]], axis=1
    )
    small = jnp.pad(small, ((0, 0), (0, 128 - small.shape[1])))
    if fused:
        turned = jnp.concatenate([query_grad, key_grad, value_grad], axis=1)
        mixed_late, turned = lax.optimization_barrier((mixed_rows, turned))
        hidden_out = (mixed_late + moe_rows.astype(f32)).astype(bf16)
        small, hidden_out, weight_last = lax.optimization_barrier(
            (small, hidden_out, weight_last)
        )
        weight_sum = weight_first + weight_last.astype(f32)
        gate_w_grad = weight_sum[:part].T[None]
        up_w_grad = weight_sum[part : 2 * part].T[None]
        down_w_grad = weight_sum[2 * part :][None]
        out_sum, query_sum, key_sum, value_sum = reduce_layer(
            normed, turned, attended, branch_grad, small, outer_count
        )
        key_width = w_key.shape[1]
        small = value_sum[:, key_width:].astype(f32)
        summed = (
            small[:, experts],
            query_sum.astype(f32),
            key_sum.astype(f32),
            value_sum[:, :key_width].astype(f32),
            out_sum.astype(f32),
            small[:, experts + 1],
            small[:, :experts],
        )
    else:
        columns = jnp.concatenate(
            [query_w_grad, key_w_grad, value_w_grad, out_w_grad, small], axis=1
        ).astype(bf16)
        hidden_out = (mixed_rows + moe_rows.astype(f32)).astype(bf16)
        shares = lax.psum_scatter(columns, everywhere, scatter_dimension=0, tiled=True)
        columns = lax.all_gather(shares, everywhere, axis=0, tiled=True).astype(f32)
        starts = [0]
        for width in (w_query.shape[1], w_key.shape[1], w_value.shape[1], model_width, experts, 1, 1):
            starts.append(starts[-1] + width)
        pieces = [columns[:, low:high] for low, high in zip(starts[:-1], starts[1:])]
        summed = (
            pieces[5][:, 0],
            pieces[0],
            pieces[1],
            pieces[2],
            pieces[3],
            pieces[6][:, 0],
            pieces[4],
        )
    return (
        hidden_out,
        grad_in,
        summed[0],
        summed[1],
        summed[2],
        summed[3],
        summed[4],
        summed[5],
        summed[6],
        gate_w_grad,
        up_w_grad,
        down_w_grad,
    )


def solution(mesh):
    names = ("outer", "inner", "narrow")
    narrow = mesh.shape["narrow"]
    cut = Mesh(mesh.devices.reshape(-1, INNER, narrow), names)
    rows = P(names, None)
    columns = P(("outer", "inner"), None, "narrow")
    depths = P(("outer", "inner"), "narrow", None)
    return jax.shard_map(
        on_device,
        mesh=cut,
        in_specs=(rows, rows, rows) + (P(),) * 7 + (columns, columns, depths, rows),
        out_specs=(rows, rows) + (P(),) * 7 + (columns, columns, depths),
        check_vma=False,
    )
```
